128 devices in a mesh: row: 16 (over y, z), col: 8 (over x, core).
Axes of the slice: x: 4, y: 4, z: 4, core: 2. Of those that a mesh axis runs over, the one named last changes fastest.
Arguments:
- features: bfloat16 [32768, 512], P(('col', 'row')), may hold values from -6 to 6
- blocks: bfloat16 [16, 8, 48, 128, 128], P('row', 'col'), may hold values from -0.375 to 0.375
- block_rows: int32 [16, 8, 48], P('row', 'col'), may hold values from 0 to 15, as said below
- block_cols: int32 [16, 8, 48], P('row', 'col'), may hold values from 0 to 31, as said below
- block_count: int32 [16, 8], P('row', 'col'), may hold values from 8 to 48, as said below
- weight: bfloat16 [512, 512], replicated, may hold values from -0.25 to 0.25
- bias_vector: float32 [512], replicated, may hold values from -4 to 4
- upstream: bfloat16 [32768, 512], P(('row', 'col')), may hold values from -6 to 6
Outputs:
- activated: bfloat16 [32768, 512], P(('row', 'col'))
- grad_weight: float32 [512, 512], replicated
- grad_bias: float32 [512], replicated
- grad_features: bfloat16 [32768, 512], P(('col', 'row'))
The draws below stay inside these ranges and needn't reach their ends.
Inputs may be any that keep to these rules, and one draw needn't show every extreme that they name: `block_rows`: the live (block row, block column) pairs of one device are distinct. `block_cols`: paired slot by slot with block_rows. `block_count`: live slots come first; some device has exactly 48 live slots.
All inputs are finite; a program needn't handle non-finite values.
Results may differ from the reference program's by a relative error of at most 0.0061.
Values may be sent and summed in bfloat16 or wider, within the bound.
A program may use at most 64 MiB of HBM per device.

```python
import jax
import jax.numpy as jnp
from jax import lax

HIDDEN_SIZE = 512
BLOCK = 128
ROW_GROUPS = 16
COL_GROUPS = 8
NODES = 32768
RB = 16
CB = 32
MAXB = 48


def block_pattern(key):
    base_key = jax.random.fold_in(key, 7)
    devices_all = ROW_GROUPS * COL_GROUPS
    band_width = max(1, CB // 8)

    def one_device(dev_key):
        weight_key, noise_key, shift_key = jax.random.split(dev_key, 3)
        row_weights = jax.random.randint(weight_key, (RB,), 1, 9)
        noise = jax.random.randint(noise_key, (RB, CB), 0, 8192)
        shift = jax.random.randint(shift_key, (), 0, CB)
        row_ids = jnp.arange(RB, dtype=jnp.int32)
        col_ids = jnp.arange(CB, dtype=jnp.int32)
        centre = (row_ids * CB // RB + shift) % CB
        offset = jnp.abs(col_ids[None, :] - centre[:, None])
        distance = jnp.minimum(offset, CB - offset)
        nearness = 1 + 7 * (distance <= band_width).astype(jnp.int32)
        scores = noise * row_weights[:, None] * nearness
        scores = scores * (RB * CB) + jnp.arange(RB * CB, dtype=jnp.int32).reshape(RB, CB)
        order = jnp.argsort(-scores.reshape(-1))
        return order[:MAXB].astype(jnp.int32)
    dev_keys = jax.random.split(base_key, devices_all)
    return jax.vmap(one_device)(dev_keys).reshape(ROW_GROUPS, COL_GROUPS, MAXB)


def draw_block_rows(key, part):
    return (block_pattern(key) // CB).astype(jnp.int32)


def draw_block_cols(key, part):
    return (block_pattern(key) % CB).astype(jnp.int32)


def draw_block_count(key, part):
    devices_all = ROW_GROUPS * COL_GROUPS
    divisor = jax.random.randint(jax.random.fold_in(key, 11), (devices_all,), 1, 7)
    counts = jnp.maximum(1, MAXB // divisor)
    fullest = jax.random.randint(jax.random.fold_in(key, 13), (), 0, devices_all)
    counts = counts.at[fullest].set(MAXB)
    return counts.reshape(ROW_GROUPS, COL_GROUPS).astype(jnp.int32)


def level_of(own_key, dims, pieces, low, largest):
    def one(axis_at, shards_of):
        heights = jax.random.uniform(jax.random.fold_in(jax.random.fold_in(own_key, 6), axis_at), (shards_of,), jnp.float32, low / len(pieces), largest / len(pieces))
        return jnp.repeat(jnp.exp(heights), dims[axis_at] // shards_of).reshape((-1,) + (1,) * (len(dims) - axis_at - 1))

    loudness = one(*pieces[0])
    for cut in pieces[1:]:
        loudness = loudness * one(*cut)
    return loudness


def bell_draw(own_key, dims, scale, most, cuts=(), held_as=jnp.bfloat16):
    drawn = scale * jax.random.normal(own_key, dims, jnp.float32)
    if cuts:
        drawn = drawn * level_of(own_key, dims, cuts, -0.22, 0.18)
    return jnp.clip(drawn, -most, most).astype(held_as)


def setup_inputs(seed: int = 0) -> dict:
    splits = jax.random.split(jax.random.key(seed), 9)
    features = bell_draw(splits[0], (NODES, HIDDEN_SIZE), 1.0, 6.0, ((0, 128),))
    blocks = bell_draw(splits[1], (ROW_GROUPS, COL_GROUPS, MAXB, BLOCK, BLOCK), ((BLOCK * MAXB * COL_GROUPS // (2 * RB)) ** -0.5), 0.375, ((0, 16), (1, 8)))
    block_rows = draw_block_rows(jax.random.fold_in(splits[8], 71), 0)
    block_cols = draw_block_cols(jax.random.fold_in(splits[8], 71), 0)
    block_count = draw_block_count(jax.random.fold_in(splits[8], 71), 0)
    weight = bell_draw(splits[5], (HIDDEN_SIZE, HIDDEN_SIZE), HIDDEN_SIZE ** -0.5, 0.25)
    bias_vector = bell_draw(splits[6], (HIDDEN_SIZE,), 1.0, 4.0, (), jnp.float32)
    upstream = bell_draw(splits[7], (NODES, HIDDEN_SIZE), 1.0, 6.0, ((0, 128),))
    return {"features": features, "blocks": blocks, "block_rows": block_rows, "block_cols": block_cols, "block_count": block_count, "weight": weight, "bias_vector": bias_vector, "upstream": upstream}


def reference(features, blocks, block_rows, block_cols, block_count, weight, bias_vector, upstream):
    node_total = features.shape[0]
    width = features.shape[1]
    devices_all = ROW_GROUPS * COL_GROUPS
    block_tiles = blocks.reshape(devices_all, MAXB, BLOCK, BLOCK)
    row_index = jnp.arange(devices_all, dtype=jnp.int32) // COL_GROUPS
    col_index = jnp.arange(devices_all, dtype=jnp.int32) % COL_GROUPS
    row_global = (row_index[:, None] * RB + block_rows.reshape(devices_all, MAXB)).astype(jnp.int32)
    col_global = (col_index[:, None] * CB + block_cols.reshape(devices_all, MAXB)).astype(jnp.int32)
    live_mask = jnp.arange(MAXB, dtype=jnp.int32)[None, :] < block_count.reshape(devices_all, 1)
    zero_blocks = jnp.zeros((node_total // BLOCK, BLOCK, width), jnp.float32)
    feature_blocks = features.reshape(node_total // BLOCK, BLOCK, width)

    def forward_one(totals, device):
        picked = feature_blocks[col_global[device]].astype(jnp.float32)
        chosen = jnp.where(live_mask[device][:, None, None], block_tiles[device], jnp.zeros_like(block_tiles[device])).astype(jnp.float32)
        product = jnp.einsum('sij,sjh->sih', chosen, picked)
        return (totals.at[row_global[device]].add(product), None)
    hidden_sum, unused = lax.scan(forward_one, zero_blocks, jnp.arange(devices_all, dtype=jnp.int32))
    hidden = hidden_sum.reshape(node_total, width).astype(jnp.bfloat16)
    preact = jnp.dot(hidden, weight, preferred_element_type=jnp.float32) + bias_vector
    sigmoid_pre = jax.nn.sigmoid(preact)
    activated = (preact * sigmoid_pre).astype(jnp.bfloat16)
    dpre = (upstream.astype(jnp.float32) * sigmoid_pre * (1.0 + preact * (1.0 - sigmoid_pre))).astype(jnp.bfloat16)
    scale_factor = 1.0 / jnp.sqrt(jnp.float32(node_total))
    grad_weight = jnp.dot(hidden.T, dpre, preferred_element_type=jnp.float32) * scale_factor
    grad_bias = lax.optimization_barrier(jnp.sum(dpre.astype(jnp.float32), axis=0)) * scale_factor
    dhidden = jnp.dot(dpre, weight.T, preferred_element_type=jnp.float32).astype(jnp.bfloat16)
    grad_blocks = dhidden.reshape(node_total // BLOCK, BLOCK, width)

    def backward_one(totals, device):
        picked = grad_blocks[row_global[device]].astype(jnp.float32)
        chosen = jnp.where(live_mask[device][:, None, None], block_tiles[device], jnp.zeros_like(block_tiles[device])).astype(jnp.float32)
        product = jnp.einsum('sji,sjh->sih', chosen, picked)
        return (totals.at[col_global[device]].add(product), None)
    grad_sum, unused = lax.scan(backward_one, zero_blocks, jnp.arange(devices_all, dtype=jnp.int32))
    grad_features = grad_sum.reshape(node_total, width).astype(jnp.bfloat16)
    return (activated, grad_weight, grad_bias, grad_features)
```

```python
import functools
import math

import jax
import jax.numpy as jnp
from jax import lax
from jax.experimental import pallas as pl
from jax.experimental.pallas import tpu as pltpu
from jax.sharding import PartitionSpec as P

MESH = pl.DeviceIdType.MESH
F32 = jnp.float32
BF16 = jnp.bfloat16
SIDE = 4
TILE = 128
WIDE = 256
CHUNKS = 2
KBLOCKS = 32
IBLOCKS = 16
SLOTS = 48
GATHER_MESSAGES = 60
MESSAGES = 168


def wrap(value):
    return value % SIDE


def at_k(h, a, b):
    a, b = wrap(a), wrap(b)
    dy, dz = (a, b) if h == 0 else (b, a)
    return (dy * SIDE + dz) * 2 + h


def step_kernel(
    scale,
    tbl,
    feat,
    blocks,
    weight,
    bias,
    ups,
    act_o,
    gf_o,
    gw_o,
    gb_o,
    G,
    BK,
    BT,
    WT,
    UP,
    PS,
    S1,
    R0,
    XS,
    XR,
    HD,
    DP,
    DG,
    TK,
    UK,
    SB,
    SR,
    GP,
    AK,
    AX,
    AXR,
    AY,
    AYR,
    AZ,
    AZR,
    FK,
    lsem,
    ssem,
    rsem,
):
    ri = lax.axis_index("row")
    ci = lax.axis_index("col")
    y, z = ri // SIDE, ri % SIDE
    x, k = ci // 2, ci % 2
    turn = 1 - 2 * k

    def dev(dy=0, dz=0, dx=0, dk=0):
        row = ((y + dy + SIDE) % SIDE) * SIDE + (z + dz + SIDE) % SIDE
        col = ((x + dx + SIDE) % SIDE) * 2 + (k + dk) % 2
        return (row, col)

    def along(h, first, step):
        if (h == 0) == first:
            return dev(dy=step)
        return dev(dz=step)

    messages = {}

    def send(key, src, dst, to, landing=None):
        number = len(messages)
        copy = pltpu.make_async_remote_copy(
            src_ref=src,
            dst_ref=dst,
            send_sem=ssem.at[number],
            recv_sem=rsem.at[number],
            device_id=to,
            device_id_type=MESH,
        )
        copy.start()
        if landing is not None:
            copy_in = pltpu.make_async_remote_copy(
                src_ref=landing,
                dst_ref=landing,
                send_sem=ssem.at[number],
                recv_sem=rsem.at[number],
                device_id=to,
                device_id_type=MESH,
            )
        else:
            copy_in = copy
        messages[key] = (copy, copy_in)

    def take(key):
        messages[key][1].wait_recv()

    local = []

    def fetch(src, dst):
        copy = pltpu.make_async_copy(src, dst, lsem.at[len(local)])
        copy.start()
        local.append(copy)
        return copy

    own = [
        [
            fetch(
                feat.at[pl.ds(h * TILE, TILE), pl.ds(c * WIDE, WIDE)],
                G.at[c, at_k(h, 0, 0)],
            )
            for h in range(2)
        ]
        for c in range(CHUNKS)
    ]
    blocks_in = fetch(blocks, BK.at[pl.ds(0, SLOTS)])
    weight_in = fetch(weight, WT)
    ups_in = fetch(ups, UP)

    barrier = pltpu.get_barrier_semaphore()
    partners = [dev(dk=1)]
    for step in (1, -1, 2):
        partners += [dev(dy=step), dev(dz=step), dev(dx=step)]
    for partner in partners:
        pl.semaphore_signal(barrier, inc=1, device_id=partner, device_id_type=MESH)
    BK[SLOTS] = jnp.zeros((TILE, TILE), BF16)
    BT[SLOTS] = jnp.zeros((TILE, TILE), BF16)
    pl.semaphore_wait(barrier, len(partners))

    def first_way(c):
        return 1 if c == 0 else -1

    def second_way(a):
        return 1 if a in (0, 1) else -1

    def second_sends(c, h, a):
        src = G.at[c, at_k(h, a, 0)]
        send(("g2p", c, h, a), src, G.at[c, at_k(h, a, -1)], along(h, False, 1))
        send(("g2m", c, h, a), src, G.at[c, at_k(h, a, 1)], along(h, False, -1))

    def gather_0(c):
        for h in range(2):
            own[c][h].wait()
        for h in range(2):
            src = G.at[c, at_k(h, 0, 0)]
            send(("g1p", c, h), src, G.at[c, at_k(h, -1, 0)], along(h, True, 1))
            send(("g1m", c, h), src, G.at[c, at_k(h, 1, 0)], along(h, True, -1))
        for h in range(2):
            second_sends(c, h, 0)

    def gather_1(c):
        e = first_way(c)
        for h in range(2):
            take(("g1p" if e == 1 else "g1m", c, h))
            send(
                ("g1r", c, h),
                G.at[c, at_k(h, -e, 0)],
                G.at[c, at_k(h, 2, 0)],
                along(h, True, e),
            )
            second_sends(c, h, -e)
        for h in range(2):
            take(("g1m" if e == 1 else "g1p", c, h))
            second_sends(c, h, e)

    def second_relay(c, h, a):
        e = second_way(a)
        take(("g2p" if e == 1 else "g2m", c, h, a))
        send(
            ("g2r", c, h, a),
            G.at[c, at_k(h, a, -e)],
            G.at[c, at_k(h, a, 2)],
            along(h, False, e),
        )

    def second_other(c, h, a):
        e = second_way(a)
        take(("g2m" if e == 1 else "g2p", c, h, a))

    def gather_2(c):
        for h in range(2):
            second_relay(c, h, 0)
        for h in range(2):
            second_other(c, h, 0)

    def gather_3(c):
        for h in range(2):
            take(("g1r", c, h))
            second_sends(c, h, 2)

    def gather_4(c):
        for a in (1, -1):
            for h in range(2):
                second_relay(c, h, a)
        for a in (1, -1):
            for h in range(2):
                second_other(c, h, a)

    def gather_5(c):
        for h in range(2):
            take(("g2r", c, h, 0))

    def gather_6(c):
        for h in range(2):
            second_relay(c, h, 2)
        for h in range(2):
            second_other(c, h, 2)

    def gather_7(c):
        for a in (1, -1):
            for h in range(2):
                take(("g2r", c, h, a))

    def gather_8(c):
        for h in range(2):
            take(("g2r", c, h, 2))

    rows_at_once = 4
    turns = IBLOCKS // rows_at_once

    def multiply(c, ks, first=False):
        @pl.loop(0, turns)
        def _(m):
            lhs = jnp.concatenate(
                [
                    jnp.concatenate(
                        [BK[tbl[kk * IBLOCKS + m * rows_at_once + j]] for kk in ks],
                        axis=1,
                    )
                    for j in range(rows_at_once)
                ],
                axis=0,
            )
            rhs = jnp.concatenate([G[c, kk] for kk in ks], axis=0)
            value = jnp.dot(lhs, rhs, preferred_element_type=F32)
            if not first:
                value = value + PS[c, m]
            PS[c, m] = value

    def halves(pairs):
        return [at_k(h, a, b) for a, b in pairs for h in range(2)]

    def multiply_own(c):
        multiply(c, halves([(0, 0)]), first=True)

    def multiply_1(c):
        multiply(c, halves([(1, 0), (-1, 0)]))

    def multiply_2(c):
        multiply(c, halves([(0, 1), (0, -1)]))

    def multiply_35(c):
        multiply(c, halves([(2, 0), (0, 2)]))

    def multiply_4(c):
        multiply(c, halves([(1, 1), (1, -1)]))
        multiply(c, halves([(-1, 1), (-1, -1)]))

    def multiply_6(c):
        multiply(c, halves([(2, 1), (2, -1)]))

    def multiply_7(c):
        multiply(c, halves([(1, 2), (-1, 2)]))

    def multiply_8(c):
        multiply(c, halves([(2, 2)]))

    def part_of(c, dk, dx):
        place = dk * SIDE + dx
        return PS[c, place // 2, pl.ds((place % 2) * 256, 256), :]

    def reduce_0(c):
        for dx in (2, 3, 1, 0):
            S1[c, dx] = part_of(c, 1, dx).astype(BF16)
            mirrored = wrap(-dx)
            send(("c0", c, mirrored), S1.at[c, dx], R0.at[c, mirrored], dev(dk=1))

    def paired(c, dx):
        take(("c0", c, dx))
        return part_of(c, 0, dx) + R0[c, dx].astype(F32)

    def reduce_1(c):
        XS[c, 0] = paired(c, 2).astype(BF16)
        send(("cf", c), XS.at[c, 0], XR.at[c, 0], dev(dx=turn))
        XS[c, 1] = paired(c, 3).astype(BF16)
        send(("cd", c), XS.at[c, 1], XR.at[c, 1], dev(dx=-turn))

    def reduce_2(c):
        value = paired(c, 1)
        take(("cf", c))
        XS[c, 2] = (value + XR[c, 0].astype(F32)).astype(BF16)
        send(("cr", c), XS.at[c, 2], XR.at[c, 2], dev(dx=turn))

    def reduce_3(c):
        value = paired(c, 0)
        take(("cd", c))
        value = value + XR[c, 1].astype(F32)
        take(("cr", c))
        value = value + XR[c, 2].astype(F32)
        HD[:, c * WIDE : (c + 1) * WIDE] = value.astype(BF16)

    def turn_blocks():
        @pl.loop(0, SLOTS)
        def _(s):
            BT[s] = BK[s].T

    gather_0(0)
    blocks_in.wait()
    multiply_own(0)
    gather_1(0)
    multiply_1(0)
    gather_0(1)
    gather_2(0)
    multiply_2(0)
    gather_3(0)
    multiply_own(1)
    gather_4(0)
    multiply_4(0)
    gather_1(1)
    gather_5(0)
    multiply_35(0)
    gather_6(0)
    gather_2(1)
    multiply_6(0)
    gather_7(0)
    multiply_7(0)
    gather_8(0)
    gather_3(1)
    multiply_8(0)
    reduce_0(0)
    multiply_1(1)
    reduce_1(0)
    gather_4(1)
    multiply_2(1)
    reduce_2(0)
    gather_5(1)
    multiply_35(1)
    gather_6(1)
    multiply_4(1)
    reduce_3(0)
    multiply_6(1)
    gather_7(1)
    multiply_7(1)
    gather_8(1)
    multiply_8(1)
    reduce_0(1)
    reduce_1(1)
    turn_blocks()
    reduce_2(1)
    weight_in.wait()
    ups_in.wait()
    reduce_3(1)

    bias_rows = []
    for n in range(CHUNKS):
        columns = slice(n * WIDE, (n + 1) * WIDE)
        pre = jnp.dot(HD[...], WT[:, columns], preferred_element_type=F32) + bias[:, columns]
        sig = jax.nn.sigmoid(pre)
        act_o[:, columns] = (pre * sig).astype(BF16)
        dpre = (UP[:, columns].astype(F32) * sig * (1.0 + pre * (1.0 - sig))).astype(BF16)
        DP[:, columns] = dpre
        bias_rows.append(jnp.sum(dpre.astype(F32).reshape(32, 8, WIDE), axis=0))

    def spread_0(c):
        value = lax.dot_general(
            DP[...],
            WT[pl.ds(c * WIDE, WIDE), :],
            (((1,), (1,)), ((), ())),
            preferred_element_type=F32,
        )
        DG[c, 0] = value.astype(BF16)
        send(("sp", c), DG.at[c, 0], DG.at[c, 3], dev(dx=turn))
        send(("sm", c), DG.at[c, 0], DG.at[c, 1], dev(dx=-turn))
        send(("sc", c, 0), DG.at[c, 0], DG.at[c, SIDE], dev(dk=1))

    def spread_1(c):
        take(("sp", c))
        send(("sr", c), DG.at[c, 3], DG.at[c, 2], dev(dx=turn))
        send(("sc", c, 1), DG.at[c, 3], DG.at[c, SIDE + 1], dev(dk=1))
        take(("sm", c))
        send(("sc", c, 2), DG.at[c, 1], DG.at[c, SIDE + 3], dev(dk=1))

    def spread_2(c):
        take(("sr", c))
        send(("sc", c, 3), DG.at[c, 2], DG.at[c, SIDE + 2], dev(dk=1))

    def spread_3(c):
        for n in range(SIDE):
            take(("sc", c, n))

    def weight_0():
        value = lax.dot_general(
            HD[...], DP[...], (((0,), (0,)), ((), ())), preferred_element_type=F32
        )
        GP[..., 0:16, :] = value.reshape(2, SIDE, SIDE, 16, 512)
        for n in range(CHUNKS):
            GP[..., 16:24, n * WIDE : (n + 1) * WIDE] = jnp.broadcast_to(
                bias_rows[n], (2, SIDE, SIDE, 8, WIDE)
            )
        send(("wk",), GP.at[1 - k], AK, dev(dk=1))

    def weight_1():
        take(("wk",))
        AX[...] = GP[k] + AK[...]
        for n in (2, 1, 3):
            send(("wx", n), AX.at[(x + n) % SIDE], AXR.at[n - 1], dev(dx=n))

    def weight_2():
        value = AX[x]
        for n in (2, 1, 3):
            take(("wx", n))
            value = value + AXR[n - 1]
        AY[...] = value
        for n in (2, 1, 3):
            send(("wy", n), AY.at[(y + n) % SIDE], AYR.at[n - 1], dev(dy=n))

    def weight_3():
        value = AY[y]
        for n in (2, 1, 3):
            take(("wy", n))
            value = value + AYR[n - 1]
        for n in range(SIDE):
            AZ[n] = value[:, n * TILE : (n + 1) * TILE]
        for n in (2, 1, 3):
            send(("wz", n), AZ.at[(z + n) % SIDE], AZR.at[n - 1], dev(dz=n))

    def weight_4():
        value = AZ[z]
        for n in (2, 1, 3):
            take(("wz", n))
            value = value + AZR[n - 1]
        FK[k, x, y, z] = value * scale
        mine = FK.at[k, x, y, z]
        for n in (2, 1, 3):
            send(("vz", n), mine, mine, dev(dz=n), FK.at[k, x, y, (z + SIDE - n) % SIDE])

    def weight_5():
        for n in (2, 1, 3):
            take(("vz", n))
        mine = FK.at[k, x, y]
        for n in (2, 1, 3):
            send(("vy", n), mine, mine, dev(dy=n), FK.at[k, x, (y + SIDE - n) % SIDE])

    def weight_6():
        for n in (2, 1, 3):
            take(("vy", n))
        mine = FK.at[k, x]
        for n in (2, 1, 3):
            send(("vx", n), mine, mine, dev(dx=n), FK.at[k, (x + SIDE - n) % SIDE])

    def weight_7():
        for n in (2, 1, 3):
            take(("vx", n))
        send(("vk",), FK.at[k], FK.at[k], dev(dk=1), FK.at[1 - k])

    def weight_8():
        take(("vk",))
        for n in range(SIDE):
            gw_o[:, n * TILE : (n + 1) * TILE] = FK[:, :, :, n, 0:16, :].reshape(512, TILE)
            gb_o[:, n * TILE : (n + 1) * TILE] = jnp.broadcast_to(
                jnp.sum(FK[0, 0, 0, n, 16:24, :], axis=0, keepdims=True), (8, TILE)
            )

    order = [(a, h) for a in ("far", "relay", "near", "mine") for h in range(2)]

    def offset(c, name):
        e = first_way(c)
        return {"far": 2, "relay": e, "near": -e, "mine": 0}[name]

    def group_way(name):
        return 1 if name in ("far", "mine") else -1

    def back_0(c, n):
        name, h = order[n]
        a, e = offset(c, name), group_way(name)
        bs = (2, -e, e, 0)
        lhs = jnp.concatenate(
            [
                jnp.concatenate(
                    [BT[tbl[at_k(h, a, b) * IBLOCKS + i]] for i in range(IBLOCKS)], axis=1
                )
                for b in bs
            ],
            axis=0,
        )
        rhs = DG[c].reshape(2048, WIDE)
        value = jnp.dot(lhs, rhs, preferred_element_type=F32)
        SB[c, n, 0:2] = value[0:256].astype(BF16).reshape(2, TILE, WIDE)
        TK[c, n] = value[256:512].reshape(2, TILE, WIDE)
        send(("bf", c, n), SB.at[c, n, 0], SR.at[c, n, 0], along(h, False, e))
        send(("bd", c, n), SB.at[c, n, 1], SR.at[c, n, 1], along(h, False, -e))

    def back_1(c, n):
        name, h = order[n]
        e = group_way(name)
        take(("bf", c, n))
        SB[c, n, 2] = (TK[c, n, 0] + SR[c, n, 0].astype(F32)).astype(BF16)
        send(("br", c, n), SB.at[c, n, 2], SR.at[c, n, 2], along(h, False, e))

    def back_2(c, n):
        name, h = order[n]
        e = first_way(c)
        take(("bd", c, n))
        value = TK[c, n, 1] + SR[c, n, 1].astype(F32)
        take(("br", c, n))
        value = value + SR[c, n, 2].astype(F32)
        late = 8 + h
        if name == "far":
            SB[c, late, 0] = value.astype(BF16)
            send(("tf", c, h), SB.at[c, late, 0], SR.at[c, late, 0], along(h, True, e))
        elif name == "near":
            SB[c, late, 1] = value.astype(BF16)
            send(("td", c, h), SB.at[c, late, 1], SR.at[c, late, 1], along(h, True, -e))
        elif name == "relay":
            take(("tf", c, h))
            SB[c, late, 2] = (value + SR[c, late, 0].astype(F32)).astype(BF16)
            send(("tr", c, h), SB.at[c, late, 2], SR.at[c, late, 2], along(h, True, e))
        else:
            UK[c, h] = value

    def back_3(c, h):
        late = 8 + h
        take(("td", c, h))
        value = UK[c, h] + SR[c, late, 1].astype(F32)
        take(("tr", c, h))
        value = value + SR[c, late, 2].astype(F32)
        gf_o[h * TILE : (h + 1) * TILE, c * WIDE : (c + 1) * WIDE] = value.astype(BF16)

    spread_0(0)
    spread_0(1)
    weight_0()
    spread_1(0)
    spread_1(1)
    spread_2(0)
    weight_1()
    spread_3(0)

    total = CHUNKS * 8
    extra = {
        1: lambda: spread_2(1),
        4: weight_2,
        7: weight_3,
        9: weight_4,
        11: weight_5,
        13: weight_6,
        17: weight_7,
    }
    for n in range(total + 4):
        if n == 8:
            spread_3(1)
        if n < total:
            back_0(n // 8, n % 8)
        if 0 <= n - 2 < total:
            back_1((n - 2) // 8, (n - 2) % 8)
        if 0 <= n - 4 < total:
            back_2((n - 4) // 8, (n - 4) % 8)
        if n in extra:
            extra[n]()
        if n == 14:
            for h in range(2):
                back_3(0, h)
    weight_8()
    for h in range(2):
        back_3(1, h)

    assert len(messages) == MESSAGES, len(messages)
    for copy, _ in messages.values():
        copy.wait_send()


def pick_table(block_rows, block_cols, block_count):
    ri = lax.axis_index("row")
    ci = lax.axis_index("col")
    y, z = ri // SIDE, ri % SIDE
    x, k = ci // 2, ci % 2
    turn = 1 - 2 * k
    place = jnp.arange(KBLOCKS * IBLOCKS, dtype=jnp.int32)
    kk, ii = place // IBLOCKS, place % IBLOCKS
    from_row = ((y + kk // 8) % SIDE) * SIDE + (z + (kk // 2) % SIDE) % SIDE
    column = from_row * 2 + kk % 2
    dk, dx = ii // 8, (ii // 2) % SIDE
    to_col = ((x + turn * dx + SIDE) % SIDE) * 2 + (k + dk) % 2
    row = to_col * 2 + ii % 2
    wanted = row * KBLOCKS + column
    slot = jnp.arange(SLOTS, dtype=jnp.int32)
    held = jnp.where(slot < block_count, block_rows * KBLOCKS + block_cols, -1)
    match = wanted[:, None] == held[None, :]
    return SLOTS + jnp.sum(jnp.where(match, slot[None, :] - SLOTS, 0), axis=1)


def shards(features, blocks, block_rows, block_cols, block_count, weight, bias_vector, upstream):
    scale = 1.0 / math.sqrt(features.shape[0] * SIDE * SIDE * SIDE * 2)
    table = pick_table(block_rows[0, 0], block_cols[0, 0], block_count[0, 0])
    vmem = pl.BlockSpec(memory_space=pltpu.VMEM)
    hbm = pl.BlockSpec(memory_space=pl.ANY)
    activated, grad_features, grad_weight, grad_bias = pl.pallas_call(
        functools.partial(step_kernel, scale),
        out_shape=(
            jax.ShapeDtypeStruct((256, 512), BF16),
            jax.ShapeDtypeStruct((256, 512), BF16),
            jax.ShapeDtypeStruct((512, 512), F32),
            jax.ShapeDtypeStruct((8, 512), F32),
        ),
        in_specs=[pl.BlockSpec(memory_space=pltpu.SMEM), hbm, hbm, hbm, vmem, hbm],
        out_specs=(vmem, vmem, vmem, vmem),
        scratch_shapes=[
            pltpu.VMEM((CHUNKS, KBLOCKS, TILE, WIDE), BF16),
            pltpu.VMEM((SLOTS + 1, TILE, TILE), BF16),
            pltpu.VMEM((SLOTS + 1, TILE, TILE), BF16),
            pltpu.VMEM((512, 512), BF16),
            pltpu.VMEM((256, 512), BF16),
            pltpu.VMEM((CHUNKS, 4, 512, WIDE), F32),
            pltpu.VMEM((CHUNKS, SIDE, 256, WIDE), BF16),
            pltpu.VMEM((CHUNKS, SIDE, 256, WIDE), BF16),
            pltpu.VMEM((CHUNKS, 3, 256, WIDE), BF16),
            pltpu.VMEM((CHUNKS, 3, 256, WIDE), BF16),
            pltpu.VMEM((256, 512), BF16),
            pltpu.VMEM((256, 512), BF16),
            pltpu.VMEM((CHUNKS, 2 * SIDE, 256, WIDE), BF16),
            pltpu.VMEM((CHUNKS, 8, 2, TILE, WIDE), F32),
            pltpu.VMEM((CHUNKS, 2, TILE, WIDE), F32),
            pltpu.VMEM((CHUNKS, 10, 3, TILE, WIDE), BF16),
            pltpu.VMEM((CHUNKS, 10, 3, TILE, WIDE), BF16),
            pltpu.VMEM((2, SIDE, SIDE, 24, 512), F32),
            pltpu.VMEM((SIDE, SIDE, 24, 512), F32),
            pltpu.VMEM((SIDE, SIDE, 24, 512), F32),
            pltpu.VMEM((3, SIDE, 24, 512), F32),
            pltpu.VMEM((SIDE, 24, 512), F32),
            pltpu.VMEM((3, 24, 512), F32),
            pltpu.VMEM((SIDE, 24, TILE), F32),
            pltpu.VMEM((3, 24, TILE), F32),
            pltpu.VMEM((2, SIDE, SIDE, SIDE, 24, TILE), F32),
            pltpu.SemaphoreType.DMA((7,)),
            pltpu.SemaphoreType.DMA((MESSAGES,)),
            pltpu.SemaphoreType.DMA((MESSAGES,)),
        ],
        compiler_params=pltpu.CompilerParams(
            collective_id=0, has_side_effects=True, vmem_limit_bytes=60 * 2**20
        ),
        name="graph_layer",
    )(table, features, blocks[0, 0], weight, bias_vector.reshape(1, 512), upstream)
    return (activated, grad_weight, grad_bias[0], grad_features)


def solution(mesh):
    in_specs = (
        P(("col", "row"), None),
        P("row", "col", None, None, None),
        P("row", "col", None),
        P("row", "col", None),
        P("row", "col"),
        P(),
        P(),
        P(("row", "col"), None),
    )
    out_specs = (P(("row", "col"), None), P(), P(), P(("col", "row"), None))
    return jax.shard_map(shards, mesh=mesh, in_specs=in_specs, out_specs=out_specs, check_vma=False)
```

```python
import functools
import math

import jax
import jax.numpy as jnp
from jax import lax
from jax.experimental import pallas as pl
from jax.experimental.pallas import tpu as pltpu
from jax.sharding import PartitionSpec as P

MESH = pl.DeviceIdType.MESH
F32 = jnp.float32
BF16 = jnp.bfloat16
SIDE = 4
TILE = 128
WIDE = 256
CHUNKS = 2
KBLOCKS = 32
IBLOCKS = 16
SLOTS = 48
SLOTS_AT_ONCE = 16
FAR = 1 << 17
GROUPS = 88


def wrap(value):
    return value % SIDE


def at_k(h, a, b):
    a, b = wrap(a), wrap(b)
    dy, dz = (a, b) if h == 0 else (b, a)
    return (dy * SIDE + dz) * 2 + h


def step_kernel(
    scale,
    count,
    rows_in,
    cols_in,
    feat,
    blocks,
    weight,
    bias,
    ups,
    act_o,
    gf_o,
    gw_o,
    gb_o,
    G0,
    G1,
    BK,
    BT,
    WT,
    UP,
    Z0,
    Z1,
    S1,
    R0,
    XS,
    XR,
    HD,
    DP,
    DG0,
    DG1,
    UK,
    SB,
    SR,
    GP,
    AK,
    PX,
    PR,
    XA,
    XB,
    FK,
    LIKE,
    AO,
    FO,
    WO,
    BO,
    IX,
    TV,
    TS,
    lsem,
    ssem,
    rsem,
):
    G, Z, DG = (G0, G1), (Z0, Z1), (DG0, DG1)
    ri = lax.axis_index("row")
    ci = lax.axis_index("col")
    y, z = ri // SIDE, ri % SIDE
    x, k = ci // 2, ci % 2
    turn = 1 - 2 * k

    def dev(dy=0, dz=0, dx=0, dk=0):
        row = ((y + dy + SIDE) % SIDE) * SIDE + (z + dz + SIDE) % SIDE
        col = ((x + dx + SIDE) % SIDE) * 2 + (k + dk) % 2
        return (row, col)

    def along(h, first, step):
        if (h == 0) == first:
            return dev(dy=step)
        return dev(dz=step)

    groups = {}

    def send(group, src, dst, to, out=None):
        number = groups.setdefault(group, len(groups))
        pltpu.make_async_remote_copy(
            src_ref=src,
            dst_ref=dst,
            send_sem=ssem.at[group[1] if out is None else out],
            recv_sem=rsem.at[number],
            device_id=to,
            device_id_type=MESH,
        ).start()

    def wait_bytes(like, sem):
        pltpu.make_async_copy(like, like, sem).wait()

    def take(group, units):
        wait_bytes(G[group[1]].at[pl.ds(0, units)], rsem.at[groups[group]])

    local = []

    def fetch(src, dst):
        copy = pltpu.make_async_copy(src, dst, lsem.at[len(local)])
        copy.start()
        local.append(copy)
        return copy

    own = [
        [
            fetch(
                feat.at[pl.ds(h * TILE, TILE), pl.ds(c * WIDE, WIDE)],
                G[c].at[at_k(h, 0, 0)],
            )
            for h in range(2)
        ]
        for c in range(CHUNKS)
    ]
    blocks_in = fetch(blocks, BK)
    weight_in = fetch(weight, WT)
    ups_in = fetch(ups, UP)

    barrier = pltpu.get_barrier_semaphore()
    partners = [dev(dk=1)]
    for step in (1, -1):
        partners += [dev(dy=step), dev(dz=step), dev(dx=step)]
    for partner in partners:
        pl.semaphore_signal(barrier, inc=1, device_id=partner, device_id_type=MESH)
    for c in range(CHUNKS):
        Z[c][SLOTS] = jnp.zeros((TILE, WIDE), F32)
    IX[...] = jnp.zeros_like(IX)
    IX[0:1, 0:SLOTS] = rows_in[...]
    IX[8:9, 0:SLOTS] = cols_in[...]
    pl.semaphore_wait(barrier, len(partners))

    def first_way(c):
        return 1 if c == 0 else -1

    def second_way(a):
        return 1 if a in (0, 1) else -1

    def second_sends(c, a):
        for h in range(2):
            src = G[c].at[at_k(h, a, 0)]
            for step in (1, -1):
                side = "in" if step == second_way(a) else "by"
                name = "all" if side == "by" and a in (1, -1) else a
                send(
                    ("g2" + side, c, name),
                    src,
                    G[c].at[at_k(h, a, -step)],
                    along(h, False, step),
                )

    def gather_0(c):
        for h in range(2):
            own[c][h].wait()
            src = G[c].at[at_k(h, 0, 0)]
            for step in (first_way(c), -first_way(c)):
                side = "in" if step == first_way(c) else "by"
                send(("g1" + side, c), src, G[c].at[at_k(h, -step, 0)], along(h, True, step))

    def gather_own(c):
        second_sends(c, 0)

    def gather_1(c):
        e = first_way(c)
        take(("g1in", c), 2)
        for h in range(2):
            send(
                ("g1r", c),
                G[c].at[at_k(h, -e, 0)],
                G[c].at[at_k(h, 2, 0)],
                along(h, True, e),
            )
        second_sends(c, -e)
        take(("g1by", c), 2)
        second_sends(c, e)

    def second_relay(c, a):
        e = second_way(a)
        take(("g2in", c, a), 2)
        for h in range(2):
            send(
                ("g2r", c, "all" if a in (1, -1) else a),
                G[c].at[at_k(h, a, -e)],
                G[c].at[at_k(h, a, 2)],
                along(h, False, e),
            )

    def gather_2(c):
        second_relay(c, 0)

    def gather_3(c):
        take(("g1r", c), 2)
        second_sends(c, 2)

    def gather_4(c):
        second_relay(c, first_way(c) * -1)
        second_relay(c, first_way(c))

    def gather_6(c):
        second_relay(c, 2)

    def gather_8(c):
        take(("g2by", c, 0), 2)
        take(("g2by", c, "all"), 4)
        take(("g2by", c, 2), 2)
        take(("g2r", c, 0), 2)
        take(("g2r", c, "all"), 4)
        take(("g2r", c, 2), 2)

    def tables_0():
        lane = lax.broadcasted_iota(jnp.int32, (TILE, TILE), 1)
        down = lax.broadcasted_iota(jnp.int32, (TILE, TILE), 0)
        rows = jnp.broadcast_to(IX[0:1, :], (TILE, TILE))
        cols = jnp.broadcast_to(IX[8:9, :], (TILE, TILE))
        live = lane < count[0, 0]
        for which, key in enumerate((rows * KBLOCKS + cols, cols * IBLOCKS + rows)):
            shift = 5 if which == 0 else 4
            key = jnp.where(live, key, FAR + lane)
            key_down = key.T
            own, other = key_down >> shift, key_down & ((1 << shift) - 1)
            less = key < key_down
            rank = jnp.sum(jnp.where(less, 1, 0), axis=1, keepdims=True)
            same = less & ((key >> shift) == own)
            keep = jnp.minimum(jnp.sum(jnp.where(same, 1, 0), axis=1, keepdims=True), 1)
            if which == 0:
                piece = other >> 1
                dy = ((piece >> 2) + SIDE - y) & 3
                dz = (piece + SIDE - z) & 3
                place = (dy * SIDE + dz) * 2 + (other & 1)
            else:
                to_col = other >> 1
                dx = (turn * ((to_col >> 1) - x)) & 3
                dk = (to_col + 2 - k) & 1
                place = (dk * SIDE + dx) * 2 + (other & 1)
            hit = rank == lane
            upto = jnp.sum(jnp.where(own <= lane, 1, 0), axis=0, keepdims=True)
            any_own = jnp.sum(jnp.where(own == lane, 1, 0), axis=0, keepdims=True)
            at = which * 8
            TV[at : at + 1, :] = jnp.sum(jnp.where(hit, down, 0), axis=0, keepdims=True)
            TV[at + 1 : at + 2, :] = jnp.sum(jnp.where(hit, place, 0), axis=0, keepdims=True)
            TV[at + 2 : at + 3, :] = jnp.sum(jnp.where(hit, keep, 0), axis=0, keepdims=True)
            TV[at + 3 : at + 4, :] = jnp.where(any_own > 0, upto - 1, SLOTS)

    def tables_1():
        copy = pltpu.make_async_copy(TV, TS, lsem.at[7])
        copy.start()
        copy.wait()

    def product(c, which, part):
        at = which * 8
        base = part * SLOTS_AT_ONCE
        total = None if part == 0 else Z[c][base - 1]
        for slot in range(base, base + SLOTS_AT_ONCE):
            place = TS[at + 1, slot]
            block = (BK if which == 0 else BT)[TS[at, slot]]
            value = jnp.dot(block, (G if which == 0 else DG)[c][place], preferred_element_type=F32)
            if total is not None:
                value = value + total * TS[at + 2, slot].astype(F32)
            Z[c][slot] = value
            total = value

    def multiply(c, part):
        product(c, 0, part)

    def multiply_back(c, part):
        product(c, 1, part)

    def part_of(c, dk, dx):
        row = (((x + turn * dx + SIDE) % SIDE) * 2 + (k + dk) % 2) * 2
        return jnp.concatenate([Z[c][TS[3, row]], Z[c][TS[3, row + 1]]], axis=0)

    def reduce_0(c):
        for dx in (2, 3, 1, 0):
            S1[c, dx] = part_of(c, 1, dx).astype(BF16)
            mirrored = wrap(-dx)
            send(("c0", c, mirrored), S1.at[c, dx], R0.at[c, mirrored], dev(dk=1))

    def paired(c, dx):
        take(("c0", c, dx), 2)
        return part_of(c, 0, dx) + R0[c, dx].astype(F32)

    def reduce_1(c):
        XS[c, 0] = paired(c, 2).astype(BF16)
        for half in range(2):
            lines = pl.ds(half * TILE, TILE)
            send(("cf", c, half), XS.at[c, 0, lines], XR.at[c, 0, lines], dev(dx=turn))
        XS[c, 1] = paired(c, 3).astype(BF16)
        send(("cd", c), XS.at[c, 1], XR.at[c, 1], dev(dx=-turn))

    def reduce_2(c):
        value = paired(c, 1)
        for half in range(2):
            lines = pl.ds(half * TILE, TILE)
            part = value[half * TILE : (half + 1) * TILE]
            take(("cf", c, half), 1)
            XS[c, 2, lines] = (part + XR[c, 0, lines].astype(F32)).astype(BF16)
            send(("cr", c), XS.at[c, 2, lines], XR.at[c, 2, lines], dev(dx=turn))

    def reduce_3(c):
        value = paired(c, 0)
        take(("cd", c), 2)
        value = value + XR[c, 1].astype(F32)
        take(("cr", c), 2)
        value = value + XR[c, 2].astype(F32)
        HD[:, c * WIDE : (c + 1) * WIDE] = value.astype(BF16)

    def turn_blocks(part):
        @pl.loop(0, SLOTS_AT_ONCE // 4)
        def _(n):
            for j in range(4):
                s = part * SLOTS_AT_ONCE + n * 4 + j
                BT[s] = BK[s].T

    gather_0(0)
    gather_own(0)
    gather_0(1)
    tables_0()
    blocks_in.wait()
    turn_blocks(0)
    tables_1()
    gather_1(0)
    gather_own(1)
    gather_2(0)
    turn_blocks(1)
    gather_1(1)
    gather_3(0)
    gather_4(0)
    turn_blocks(2)
    gather_2(1)
    gather_6(0)
    gather_3(1)
    gather_8(0)
    multiply(0, 0)
    gather_4(1)
    multiply(0, 1)
    multiply(0, 2)
    reduce_0(0)
    gather_6(1)
    reduce_1(0)
    reduce_2(0)
    gather_8(1)
    multiply(1, 0)
    multiply(1, 1)
    multiply(1, 2)
    reduce_0(1)
    reduce_3(0)
    reduce_1(1)
    reduce_2(1)
    weight_in.wait()
    ups_in.wait()
    reduce_3(1)

    bias_rows = []
    for n in range(CHUNKS):
        columns = slice(n * WIDE, (n + 1) * WIDE)
        pre = jnp.dot(HD[...], WT[:, columns], preferred_element_type=F32) + bias[:, columns]
        sig = jax.nn.sigmoid(pre)
        AO[:, columns] = (pre * sig).astype(BF16)
        dpre = (UP[:, columns].astype(F32) * sig * (1.0 + pre * (1.0 - sig))).astype(BF16)
        DP[:, columns] = dpre
        bias_rows.append(jnp.sum(dpre.astype(F32).reshape(32, 8, WIDE), axis=0))

    def hidden(c, place):
        return DG[c].at[pl.ds(2 * place, 2)]

    def spread_0(c):
        value = lax.dot_general(
            DP[...],
            WT[pl.ds(c * WIDE, WIDE), :],
            (((1,), (1,)), ((), ())),
            preferred_element_type=F32,
        )
        DG[c][0:2] = value.astype(BF16).reshape(2, TILE, WIDE)
        for half in range(2):
            send(("sp", c, half), DG[c].at[half], DG[c].at[6 + half], dev(dx=turn))
        send(("sm", c), hidden(c, 0), hidden(c, 1), dev(dx=-turn))
        send(("sc", c), hidden(c, 0), hidden(c, SIDE), dev(dk=1))

    def spread_1(c):
        for half in range(2):
            take(("sp", c, half), 1)
            send(("sr", c), DG[c].at[6 + half], DG[c].at[4 + half], dev(dx=turn))
        send(("sc", c), hidden(c, 3), hidden(c, SIDE + 1), dev(dk=1))
        take(("sm", c), 2)
        send(("sc", c), hidden(c, 1), hidden(c, SIDE + 3), dev(dk=1))

    def spread_2(c):
        take(("sr", c), 2)
        send(("sc", c), hidden(c, 2), hidden(c, SIDE + 2), dev(dk=1))

    def spread_3(c):
        take(("sc", c), 8)

    plane = [(dy, dz) for dy in range(SIDE) for dz in range(SIDE) if dy or dz]

    def weight_0():
        value = lax.dot_general(
            HD[...], DP[...], (((0,), (0,)), ((), ())), preferred_element_type=F32
        )
        for zz in range(SIDE):
            lanes = slice(zz * TILE, (zz + 1) * TILE)
            tiles = value[:, lanes].reshape(2, SIDE, SIDE, 16, TILE)
            sums = bias_rows[zz // 2][:, (zz % 2) * TILE : (zz % 2 + 1) * TILE]
            for yy in range(SIDE):
                GP[:, yy * SIDE + zz, :, 0:16, :] = tiles[:, :, yy]
                GP[:, yy * SIDE + zz, :, 16:24, :] = jnp.broadcast_to(
                    sums, (2, SIDE, 8, TILE)
                )
        send(("wk",), GP.at[1 - k], AK, dev(dk=1), out=2)

    def weight_1():
        wait_bytes(AK, rsem.at[groups[("wk",)]])
        AK[...] = GP[k] + AK[...]
        PX[...] = AK[...].astype(BF16)
        for n, (dy, dz) in enumerate(plane):
            there = ((y + dy) % SIDE) * SIDE + (z + dz) % SIDE
            send(("wp",), PX.at[there], PR.at[n], dev(dy=dy, dz=dz), out=3)

    def weight_2():
        wait_bytes(PR, rsem.at[groups[("wp",)]])
        value = AK[ri]
        for n in range(len(plane)):
            value = value + PR[n].astype(F32)
        XA[...] = value
        for n in (2, 1, 3):
            send(("wx",), XA.at[(x + n) % SIDE], XB.at[n - 1], dev(dx=n), out=4)

    def weight_3():
        wait_bytes(XB, rsem.at[groups[("wx",)]])
        value = XA[x]
        for n in range(3):
            value = value + XB[n]
        FK[k, x, ri] = (value * scale).astype(BF16)
        mine = FK.at[k, x, ri]
        for dy, dz in plane:
            send(("vp",), mine, mine, dev(dy=dy, dz=dz), out=5)

    def weight_4():
        wait_bytes(LIKE, rsem.at[groups[("vp",)]])
        mine = FK.at[k, x]
        for n in (2, 1, 3):
            send(("vx",), mine, mine, dev(dx=n), out=6)

    def weight_5():
        wait_bytes(FK.at[0, pl.ds(0, 3)], rsem.at[groups[("vx",)]])
        send(("vk",), FK.at[k], FK.at[k], dev(dk=1), out=7)

    def weight_6():
        wait_bytes(FK.at[0], rsem.at[groups[("vk",)]])
        for yy in range(SIDE):
            for zz in range(SIDE):
                lanes = slice(zz * TILE, (zz + 1) * TILE)
                for kk in range(2):
                    for xx in range(SIDE):
                        first = kk * 256 + xx * 64 + yy * 16
                        WO[first : first + 16, lanes] = FK[kk, xx, yy * SIDE + zz, 0:16, :].astype(F32)
        for zz in range(SIDE):
            BO[:, zz * TILE : (zz + 1) * TILE] = jnp.sum(
                FK[0, 0, zz, 16:24, :].astype(F32), axis=0, keepdims=True
            )

    def offset(c, name):
        e = first_way(c)
        return {"far": 2, "relay": e, "near": -e, "mine": 0}[name]

    def group_way(name):
        return 1 if name in ("far", "mine") else -1

    def sum_of(c, h, a, b):
        dy, dz = (a, b) if h == 0 else (b, a)
        column = (((y + dy + SIDE) % SIDE) * SIDE + (z + dz + SIDE) % SIDE) * 2 + h
        return Z[c][TS[8 + 3, column]]

    NAMES = ("far", "relay", "near", "mine")

    def back_0(c, i):
        name = NAMES[i]
        a, e = offset(c, name), group_way(name)
        for h in range(2):
            SB[c, h, i, 0] = sum_of(c, h, a, 2).astype(BF16)
            send(("bf", c, i), SB.at[c, h, i, 0], SR.at[c, h, i, 0], along(h, False, e))
        for h in range(2):
            SB[c, h, i, 1] = sum_of(c, h, a, -e).astype(BF16)
            send(("bd", c, i), SB.at[c, h, i, 1], SR.at[c, h, i, 1], along(h, False, -e))

    def back_1(c, i):
        name = NAMES[i]
        a, e = offset(c, name), group_way(name)
        take(("bf", c, i), 2)
        for h in range(2):
            SB[c, h, i, 2] = (sum_of(c, h, a, e) + SR[c, h, i, 0].astype(F32)).astype(BF16)
            send(("br", c, i), SB.at[c, h, i, 2], SR.at[c, h, i, 2], along(h, False, e))

    def back_2(c, i):
        name = NAMES[i]
        e = first_way(c)
        take(("bd", c, i), 2)
        take(("br", c, i), 2)
        if name == "relay":
            take(("tf", c), 2)
        for h in range(2):
            value = sum_of(c, h, offset(c, name), 0) + SR[c, h, i, 1].astype(F32)
            value = value + SR[c, h, i, 2].astype(F32)
            if name == "far":
                SB[c, h, 4, 0] = value.astype(BF16)
                send(("tf", c), SB.at[c, h, 4, 0], SR.at[c, h, 4, 0], along(h, True, e))
            elif name == "near":
                SB[c, h, 4, 1] = value.astype(BF16)
                send(("td", c), SB.at[c, h, 4, 1], SR.at[c, h, 4, 1], along(h, True, -e))
            elif name == "relay":
                SB[c, h, 4, 2] = (value + SR[c, h, 4, 0].astype(F32)).astype(BF16)
                send(("tr", c), SB.at[c, h, 4, 2], SR.at[c, h, 4, 2], along(h, True, e))
            else:
                UK[c, h] = value

    def back_3(c):
        take(("td", c), 2)
        take(("tr", c), 2)
        for h in range(2):
            value = UK[c, h] + SR[c, h, 4, 1].astype(F32)
            value = value + SR[c, h, 4, 2].astype(F32)
            FO[h * TILE : (h + 1) * TILE, c * WIDE : (c + 1) * WIDE] = value.astype(BF16)

    out = []

    def leave(src, dst):
        copy = pltpu.make_async_copy(src, dst, lsem.at[8 + len(out)])
        copy.start()
        out.append(copy)

    spread_0(0)
    weight_0()
    leave(AO, act_o)
    spread_1(0)
    spread_0(1)
    weight_1()
    spread_2(0)
    spread_3(0)
    for part in range(3):
        multiply_back(0, part)
    for i in range(4):
        back_0(0, i)
    spread_1(1)
    weight_2()
    spread_2(1)
    back_1(0, 0)
    back_1(0, 1)
    spread_3(1)
    for part in range(3):
        multiply_back(1, part)
    back_0(1, 0)
    back_1(0, 2)
    back_0(1, 1)
    back_2(0, 0)
    back_1(0, 3)
    back_0(1, 2)
    back_2(0, 1)
    back_0(1, 3)
    weight_3()
    back_1(1, 0)
    back_2(0, 2)
    back_2(0, 3)
    back_1(1, 1)
    back_1(1, 2)
    back_3(0)
    leave(FO.at[:, pl.ds(0, WIDE)], gf_o.at[:, pl.ds(0, WIDE)])
    back_2(1, 0)
    back_1(1, 3)
    weight_4()
    back_2(1, 1)
    back_2(1, 2)
    back_2(1, 3)
    weight_5()
    weight_6()
    leave(WO, gw_o)
    leave(BO, gb_o)
    back_3(1)
    leave(FO.at[:, pl.ds(WIDE, WIDE)], gf_o.at[:, pl.ds(WIDE, WIDE)])
    for copy in out:
        copy.wait()

    assert len(groups) == GROUPS, len(groups)
    for c in range(CHUNKS):
        wait_bytes(Z[c].at[pl.ds(0, 44)], ssem.at[c])
    for number, like in enumerate(
        (AK, PR, XB, LIKE, FK.at[0, pl.ds(0, 3)], FK.at[0]), start=CHUNKS
    ):
        wait_bytes(like, ssem.at[number])


def finish_kernel(a, b, c, d, ao, bo, co, do, av, bv, cv, dv, sem):
    pairs = ((c, cv, co), (a, av, ao), (b, bv, bo), (d, dv, do))
    copies_in = [pltpu.make_async_copy(p[0], p[1], sem.at[n]) for n, p in enumerate(pairs)]
    copies_out = [pltpu.make_async_copy(p[1], p[2], sem.at[4 + n]) for n, p in enumerate(pairs)]
    for copy in copies_in:
        copy.start()
    for copy_in, copy_out in zip(copies_in, copies_out):
        copy_in.wait()
        copy_out.start()
    for copy in copies_out:
        copy.wait()


def shards(features, blocks, block_rows, block_cols, block_count, weight, bias_vector, upstream):
    scale = 1.0 / math.sqrt(features.shape[0] * SIDE * SIDE * SIDE * 2)
    vmem = pl.BlockSpec(memory_space=pltpu.VMEM)
    hbm = pl.BlockSpec(memory_space=pl.ANY)
    smem = pl.BlockSpec(memory_space=pltpu.SMEM)
    shapes = (
        jax.ShapeDtypeStruct((256, 512), BF16),
        jax.ShapeDtypeStruct((256, 512), BF16),
        jax.ShapeDtypeStruct((512, 512), F32),
        jax.ShapeDtypeStruct((1, 512), F32),
    )
    results = pl.pallas_call(
        functools.partial(step_kernel, scale),
        out_shape=shapes,
        in_specs=[smem, vmem, vmem, hbm, hbm, hbm, vmem, hbm],
        out_specs=(hbm, hbm, hbm, hbm),
        scratch_shapes=[
            pltpu.VMEM((KBLOCKS, TILE, WIDE), BF16),
            pltpu.VMEM((KBLOCKS, TILE, WIDE), BF16),
            pltpu.VMEM((SLOTS, TILE, TILE), BF16),
            pltpu.VMEM((SLOTS, TILE, TILE), BF16),
            pltpu.VMEM((512, 512), BF16),
            pltpu.VMEM((256, 512), BF16),
            pltpu.VMEM((SLOTS + 1, TILE, WIDE), F32),
            pltpu.VMEM((SLOTS + 1, TILE, WIDE), F32),
            pltpu.VMEM((CHUNKS, SIDE, 256, WIDE), BF16),
            pltpu.VMEM((CHUNKS, SIDE, 256, WIDE), BF16),
            pltpu.VMEM((CHUNKS, 3, 256, WIDE), BF16),
            pltpu.VMEM((CHUNKS, 3, 256, WIDE), BF16),
            pltpu.VMEM((256, 512), BF16),
            pltpu.VMEM((256, 512), BF16),
            pltpu.VMEM((IBLOCKS, TILE, WIDE), BF16),
            pltpu.VMEM((IBLOCKS, TILE, WIDE), BF16),
            pltpu.VMEM((CHUNKS, 2, TILE, WIDE), F32),
            pltpu.VMEM((CHUNKS, 2, 5, 3, TILE, WIDE), BF16),
            pltpu.VMEM((CHUNKS, 2, 5, 3, TILE, WIDE), BF16),
            pltpu.VMEM((2, 16, SIDE, 24, TILE), F32),
            pltpu.VMEM((16, SIDE, 24, TILE), F32),
            pltpu.VMEM((16, SIDE, 24, TILE), BF16),
            pltpu.VMEM((15, SIDE, 24, TILE), BF16),
            pltpu.VMEM((SIDE, 24, TILE), F32),
            pltpu.VMEM((3, 24, TILE), F32),
            pltpu.VMEM((2, SIDE, 16, 24, TILE), BF16),
            pltpu.VMEM((15, 24, TILE), BF16),
            pltpu.VMEM((256, 512), BF16),
            pltpu.VMEM((256, 512), BF16),
            pltpu.VMEM((512, 512), F32),
            pltpu.VMEM((1, 512), F32),
            pltpu.VMEM((16, TILE), jnp.int32),
            pltpu.VMEM((16, TILE), jnp.int32),
            pltpu.SMEM((16, TILE), jnp.int32),
            pltpu.SemaphoreType.DMA((13,)),
            pltpu.SemaphoreType.DMA((CHUNKS + 6,)),
            pltpu.SemaphoreType.DMA((GROUPS,)),
        ],
        compiler_params=pltpu.CompilerParams(
            collective_id=0, has_side_effects=True, vmem_limit_bytes=60 * 2**20
        ),
        name="graph_layer",
    )(
        block_count,
        block_rows[0],
        block_cols[0],
        features,
        blocks[0, 0],
        weight,
        bias_vector.reshape(1, 512),
        upstream,
    )
    activated, grad_features, grad_weight, grad_bias = pl.pallas_call(
        finish_kernel,
        out_shape=shapes,
        in_specs=[hbm] * 4,
        out_specs=(hbm,) * 4,
        scratch_shapes=[pltpu.VMEM(s.shape, s.dtype) for s in shapes]
        + [pltpu.SemaphoreType.DMA((8,))],
        compiler_params=pltpu.CompilerParams(vmem_limit_bytes=60 * 2**20),
        name="finish",
    )(*results)
    return (activated, grad_weight, grad_bias.reshape(512), grad_features)


def solution(mesh):
    in_specs = (
        P(("col", "row"), None),
        P("row", "col", None, None, None),
        P("row", "col", None),
        P("row", "col", None),
        P("row", "col"),
        P(),
        P(),
        P(("row", "col"), None),
    )
    out_specs = (P(("row", "col"), None), P(), P(), P(("col", "row"), None))
    return jax.shard_map(shards, mesh=mesh, in_specs=in_specs, out_specs=out_specs, check_vma=False)
```

```python
import functools
import math

import jax
import jax.numpy as jnp
from jax import lax
from jax.experimental import pallas as pl
from jax.experimental.pallas import tpu as pltpu
from jax.sharding import PartitionSpec as P

MESH = pl.DeviceIdType.MESH
F32 = jnp.float32
BF16 = jnp.bfloat16
SIDE = 4
TILE = 128
WIDE = 256
CHUNKS = 2
HALF = 256
KBLOCKS = 32
IBLOCKS = 16
SLOTS = 48
SLOTS_AT_ONCE = 16
LOCAL = 2 * CHUNKS + 6
FORWARD = (
    ("g0", 0),
    ("own", 0),
    ("g0", 1),
    ("prep",),
    ("g1", 0),
    ("own", 1),
    ("g2", 0),
    ("turn", 1),
    ("g1", 1),
    ("g3", 0),
    ("g4", 0),
    ("g2", 1),
    ("g3", 1),
    ("turn", 2),
    ("g6", 0),
    ("g4", 1),
    ("g6", 1),
    ("mm", 0),
    ("r1", 0),
    ("mm", 1),
    ("r2", 0),
    ("r1", 1),
    ("r3", 0),
    ("r2", 1),
    ("r3", 1),
)
BACKWARD = (
    ("s0", 0),
    ("w0",),
    ("s1", 0),
    ("s0", 1),
    ("w1",),
    ("s2", 0),
    ("mm", 0),
    ("b0", 0, 0),
    ("b0", 0, 1),
    ("b0", 0, 2),
    ("b0", 0, 3),
    ("s1", 1),
    ("w2",),
    ("s2", 1),
    ("b1", 0, 0),
    ("b1", 0, 1),
    ("mm", 1),
    ("b0", 1, 0),
    ("b1", 0, 2),
    ("b0", 1, 1),
    ("b1", 0, 3),
    ("w3",),
    ("b2", 0, 0),
    ("b0", 1, 2),
    ("b0", 1, 3),
    ("b1", 1, 0),
    ("b2", 0, 2),
    ("b1", 1, 1),
    ("b2", 0, 1),
    ("b1", 1, 2),
    ("w4",),
    ("b2", 1, 0),
    ("b1", 1, 3),
    ("b2", 0, 3),
    ("b2", 1, 2),
    ("b2", 1, 1),
    ("b3", 0),
    ("w5",),
    ("b2", 1, 3),
    ("w6",),
    ("b3", 1),
)
FAR = 1 << 17
GROUPS = 41 * CHUNKS + 6


def wrap(value):
    return value % SIDE


def at_k(h, a, b):
    a, b = wrap(a), wrap(b)
    dy, dz = (a, b) if h == 0 else (b, a)
    return (dy * SIDE + dz) * 2 + h


def step_kernel(scale, count, rows_in, cols_in, feat, blocks, weight, bias, ups, *refs):
    AO, FO, WO, BO = refs[:4]
    refs = refs[4:]
    G, Z, DG = refs[:CHUNKS], refs[CHUNKS : 2 * CHUNKS], refs[2 * CHUNKS : 3 * CHUNKS]
    BK, BT, WT, UP, S1, R0, XS, XR, HD, DP, UK, SB, SR = refs[3 * CHUNKS : 3 * CHUNKS + 13]
    GP, AK, PX, PR, XA, XB, FK, LIKE = refs[3 * CHUNKS + 13 : 3 * CHUNKS + 21]
    RV, CV, BV, IX, TV, TS, lsem, ssem, rsem = refs[3 * CHUNKS + 21 :]
    ri = lax.axis_index("row")
    ci = lax.axis_index("col")
    y, z = ri // SIDE, ri % SIDE
    x, k = ci // 2, ci % 2
    turn = 1 - 2 * k

    def dev(dy=0, dz=0, dx=0, dk=0):
        row = ((y + dy + SIDE) % SIDE) * SIDE + (z + dz + SIDE) % SIDE
        col = ((x + dx + SIDE) % SIDE) * 2 + (k + dk) % 2
        return (row, col)

    def along(h, first, step):
        if (h == 0) == first:
            return dev(dy=step)
        return dev(dz=step)

    groups = {}

    def send(group, src, dst, to, out=None):
        number = groups.setdefault(group, len(groups))
        pltpu.make_async_remote_copy(
            src_ref=src,
            dst_ref=dst,
            send_sem=ssem.at[group[1] if out is None else out],
            recv_sem=rsem.at[number],
            device_id=to,
            device_id_type=MESH,
        ).start()

    def wait_bytes(like, sem):
        pltpu.make_async_copy(like, like, sem).wait()

    def take(group, units):
        wait_bytes(G[group[1]].at[pl.ds(0, units)], rsem.at[groups[group]])

    local = []

    def fetch(src, dst):
        copy = pltpu.make_async_copy(src, dst, lsem.at[len(local)])
        copy.start()
        local.append(copy)
        return copy

    own = [
        [
            fetch(
                feat.at[pl.ds(h * TILE, TILE), pl.ds(c * WIDE, WIDE)],
                G[c].at[at_k(h, 0, 0)],
            )
            for h in range(2)
        ]
        for c in range(CHUNKS)
    ]
    blocks_in = fetch(blocks, BK)
    weight_in = fetch(weight, WT)
    rows_got = fetch(rows_in, RV)
    cols_got = fetch(cols_in, CV)
    ups_in = fetch(ups, UP)
    bias_in = fetch(bias, BV)

    barrier = pltpu.get_barrier_semaphore()
    partners = [dev(dk=1)]
    for step in (1, -1):
        partners += [dev(dy=step), dev(dz=step), dev(dx=step)]
    for partner in partners:
        pl.semaphore_signal(barrier, inc=1, device_id=partner, device_id_type=MESH)
    for c in range(CHUNKS):
        Z[c][SLOTS] = jnp.zeros((TILE, WIDE), F32)
    IX[...] = jnp.zeros_like(IX)
    pl.semaphore_wait(barrier, len(partners))

    def first_way(c):
        return 1 if c % 2 == 0 else -1

    def second_way(a):
        return 1 if a in (0, 1) else -1

    def second_sends(c, a):
        for h in range(2):
            src = G[c].at[at_k(h, a, 0)]
            for step in (1, -1):
                side = "in" if step == second_way(a) else "by"
                name = "all" if side == "by" and a in (1, -1) else a
                send(
                    ("g2" + side, c, name),
                    src,
                    G[c].at[at_k(h, a, -step)],
                    along(h, False, step),
                )

    def gather_0(c):
        for h in range(2):
            own[c][h].wait()
            src = G[c].at[at_k(h, 0, 0)]
            for step in (first_way(c), -first_way(c)):
                side = "in" if step == first_way(c) else "by"
                send(("g1" + side, c), src, G[c].at[at_k(h, -step, 0)], along(h, True, step))

    def gather_own(c):
        second_sends(c, 0)

    def gather_1(c):
        e = first_way(c)
        take(("g1in", c), 2)
        for h in range(2):
            send(
                ("g1r", c),
                G[c].at[at_k(h, -e, 0)],
                G[c].at[at_k(h, 2, 0)],
                along(h, True, e),
            )
        second_sends(c, -e)
        take(("g1by", c), 2)
        second_sends(c, e)

    def second_relay(c, a):
        e = second_way(a)
        take(("g2in", c, a), 2)
        for h in range(2):
            send(
                ("g2r", c, "all" if a in (1, -1) else a),
                G[c].at[at_k(h, a, -e)],
                G[c].at[at_k(h, a, 2)],
                along(h, False, e),
            )

    def gather_2(c):
        second_relay(c, 0)

    def gather_3(c):
        take(("g1r", c), 2)
        second_sends(c, 2)

    def gather_4(c):
        second_relay(c, first_way(c) * -1)
        second_relay(c, first_way(c))

    def gather_6(c):
        second_relay(c, 2)

    def gather_8(c):
        take(("g2by", c, 0), 2)
        take(("g2by", c, "all"), 4)
        take(("g2by", c, 2), 2)
        take(("g2r", c, 0), 2)
        take(("g2r", c, "all"), 4)
        take(("g2r", c, 2), 2)

    def tables_0():
        rows_got.wait()
        cols_got.wait()
        IX[0:1, 0:SLOTS] = RV[...]
        IX[8:9, 0:SLOTS] = CV[...]
        lane = lax.broadcasted_iota(jnp.int32, (TILE, TILE), 1)
        down = lax.broadcasted_iota(jnp.int32, (TILE, TILE), 0)
        rows = jnp.broadcast_to(IX[0:1, :], (TILE, TILE))
        cols = jnp.broadcast_to(IX[8:9, :], (TILE, TILE))
        live = lane < count[0, 0]
        for which, key in enumerate((rows * KBLOCKS + cols, cols * IBLOCKS + rows)):
            shift = 5 if which == 0 else 4
            key = jnp.where(live, key, FAR + lane)
            key_down = key.T
            own, other = key_down >> shift, key_down & ((1 << shift) - 1)
            less = key < key_down
            rank = jnp.sum(jnp.where(less, 1, 0), axis=1, keepdims=True)
            same = less & ((key >> shift) == own)
            keep = jnp.minimum(jnp.sum(jnp.where(same, 1, 0), axis=1, keepdims=True), 1)
            if which == 0:
                piece = other >> 1
                dy = ((piece >> 2) + SIDE - y) & 3
                dz = (piece + SIDE - z) & 3
                place = (dy * SIDE + dz) * 2 + (other & 1)
            else:
                to_col = other >> 1
                dx = (turn * ((to_col >> 1) - x)) & 3
                dk = (to_col + 2 - k) & 1
                place = (dk * SIDE + dx) * 2 + (other & 1)
            hit = rank == lane
            upto = jnp.sum(jnp.where(own <= lane, 1, 0), axis=0, keepdims=True)
            any_own = jnp.sum(jnp.where(own == lane, 1, 0), axis=0, keepdims=True)
            at = which * 8
            TV[at : at + 1, :] = jnp.sum(jnp.where(hit, down, 0), axis=0, keepdims=True)
            TV[at + 1 : at + 2, :] = jnp.sum(jnp.where(hit, place, 0), axis=0, keepdims=True)
            TV[at + 2 : at + 3, :] = jnp.sum(jnp.where(hit, keep, 0), axis=0, keepdims=True)
            TV[at + 3 : at + 4, :] = jnp.where(any_own > 0, upto - 1, SLOTS)

    def tables_1():
        copy = pltpu.make_async_copy(TV, TS, lsem.at[LOCAL])
        copy.start()
        copy.wait()

    def product(c, which, part):
        at = which * 8
        base = part * SLOTS_AT_ONCE
        total = None if part == 0 else Z[c][base - 1]
        for slot in range(base, base + SLOTS_AT_ONCE):
            place = TS[at + 1, slot]
            block = (BK if which == 0 else BT)[TS[at, slot]]
            value = jnp.dot(block, (G if which == 0 else DG)[c][place], preferred_element_type=F32)
            if total is not None:
                value = value + total * TS[at + 2, slot].astype(F32)
            Z[c][slot] = value
            total = value

    def multiply(c, part):
        product(c, 0, part)

    def multiply_back(c, part):
        product(c, 1, part)

    def part_of(c, dk, dx):
        row = (((x + turn * dx + SIDE) % SIDE) * 2 + (k + dk) % 2) * 2
        return jnp.concatenate([Z[c][TS[3, row]], Z[c][TS[3, row + 1]]], axis=0)

    def reduce_0(c):
        for dx in (2, 3, 1, 0):
            S1[c, dx] = part_of(c, 1, dx).astype(BF16)
            mirrored = wrap(-dx)
            send(("c0", c, mirrored), S1.at[c, dx], R0.at[c, mirrored], dev(dk=1))

    def paired(c, dx):
        take(("c0", c, dx), 2)
        return part_of(c, 0, dx) + R0[c, dx].astype(F32)

    def reduce_1(c):
        XS[c, 0] = paired(c, 2).astype(BF16)
        for half in range(2):
            lines = pl.ds(half * TILE, TILE)
            send(("cf", c, half), XS.at[c, 0, lines], XR.at[c, 0, lines], dev(dx=turn))
        XS[c, 1] = paired(c, 3).astype(BF16)
        send(("cd", c), XS.at[c, 1], XR.at[c, 1], dev(dx=-turn))

    def reduce_2(c):
        value = paired(c, 1)
        for half in range(2):
            lines = pl.ds(half * TILE, TILE)
            part = value[half * TILE : (half + 1) * TILE]
            take(("cf", c, half), 1)
            XS[c, 2, lines] = (part + XR[c, 0, lines].astype(F32)).astype(BF16)
            send(("cr", c), XS.at[c, 2, lines], XR.at[c, 2, lines], dev(dx=turn))

    def reduce_3(c):
        value = paired(c, 0)
        take(("cd", c), 2)
        value = value + XR[c, 1].astype(F32)
        take(("cr", c), 2)
        value = value + XR[c, 2].astype(F32)
        HD[:, c * WIDE : (c + 1) * WIDE] = value.astype(BF16)

    def turn_blocks(part):
        @pl.loop(0, SLOTS_AT_ONCE // 4)
        def _(n):
            for j in range(4):
                s = part * SLOTS_AT_ONCE + n * 4 + j
                BT[s] = BK[s].T

    def run(order, table):
        for name, *args in order:
            table[name](*args)

    def prepare():
        tables_0()
        blocks_in.wait()
        turn_blocks(0)
        tables_1()

    def multiply_all(c):
        gather_8(c)
        for part in range(3):
            multiply(c, part)
        reduce_0(c)

    steps = dict(g0=gather_0, own=gather_own, g1=gather_1, g2=gather_2, g3=gather_3, g4=gather_4)
    steps.update(g6=gather_6, mm=multiply_all, r1=reduce_1, r2=reduce_2, r3=reduce_3)
    steps.update(prep=prepare, turn=turn_blocks)
    run(FORWARD, steps)
    weight_in.wait()
    ups_in.wait()

    bias_rows = []
    bias_in.wait()
    for n in range(2):
        columns = slice(n * HALF, (n + 1) * HALF)
        pre = jnp.dot(HD[...], WT[:, columns], preferred_element_type=F32) + BV[:, columns]
        sig = jax.nn.sigmoid(pre)
        AO[:, columns] = (pre * sig).astype(BF16)
        dpre = (UP[:, columns].astype(F32) * sig * (1.0 + pre * (1.0 - sig))).astype(BF16)
        DP[:, columns] = dpre
        bias_rows.append(jnp.sum(dpre.astype(F32).reshape(32, 8, HALF), axis=0))

    def hidden(c, place):
        return DG[c].at[pl.ds(2 * place, 2)]

    def spread_0(c):
        value = lax.dot_general(
            DP[...],
            WT[pl.ds(c * WIDE, WIDE), :],
            (((1,), (1,)), ((), ())),
            preferred_element_type=F32,
        )
        DG[c][0:2] = value.astype(BF16).reshape(2, TILE, WIDE)
        for half in range(2):
            send(("sp", c, half), DG[c].at[half], DG[c].at[6 + half], dev(dx=turn))
        send(("sm", c), hidden(c, 0), hidden(c, 1), dev(dx=-turn))
        send(("sc", c), hidden(c, 0), hidden(c, SIDE), dev(dk=1))

    def spread_1(c):
        for half in range(2):
            take(("sp", c, half), 1)
            send(("sr", c), DG[c].at[6 + half], DG[c].at[4 + half], dev(dx=turn))
        send(("sc", c), hidden(c, 3), hidden(c, SIDE + 1), dev(dk=1))
        take(("sm", c), 2)
        send(("sc", c), hidden(c, 1), hidden(c, SIDE + 3), dev(dk=1))

    def spread_2(c):
        take(("sr", c), 2)
        send(("sc", c), hidden(c, 2), hidden(c, SIDE + 2), dev(dk=1))

    def spread_3(c):
        take(("sc", c), 8)

    plane = [(dy, dz) for dy in range(SIDE) for dz in range(SIDE) if dy or dz]

    def weight_0():
        value = lax.dot_general(
            HD[...], DP[...], (((0,), (0,)), ((), ())), preferred_element_type=F32
        )
        for zz in range(SIDE):
            lanes = slice(zz * TILE, (zz + 1) * TILE)
            tiles = value[:, lanes].reshape(2, SIDE, SIDE, 16, TILE)
            sums = bias_rows[zz // 2][:, (zz % 2) * TILE : (zz % 2 + 1) * TILE]
            for yy in range(SIDE):
                GP[:, yy * SIDE + zz, :, 0:16, :] = tiles[:, :, yy]
                GP[:, yy * SIDE + zz, :, 16:24, :] = jnp.broadcast_to(
                    sums, (2, SIDE, 8, TILE)
                )
        send(("wk",), GP.at[1 - k], AK, dev(dk=1), out=CHUNKS + 0)

    def weight_1():
        wait_bytes(AK, rsem.at[groups[("wk",)]])
        AK[...] = GP[k] + AK[...]
        PX[...] = AK[...].astype(BF16)
        for n, (dy, dz) in enumerate(plane):
            there = ((y + dy) % SIDE) * SIDE + (z + dz) % SIDE
            send(("wp",), PX.at[there], PR.at[n], dev(dy=dy, dz=dz), out=CHUNKS + 1)

    def weight_2():
        wait_bytes(PR, rsem.at[groups[("wp",)]])
        value = AK[ri]
        for n in range(len(plane)):
            value = value + PR[n].astype(F32)
        XA[...] = value
        for n in (2, 1, 3):
            send(("wx",), XA.at[(x + n) % SIDE], XB.at[n - 1], dev(dx=n), out=CHUNKS + 2)

    def weight_3():
        wait_bytes(XB, rsem.at[groups[("wx",)]])
        value = XA[x]
        for n in range(3):
            value = value + XB[n]
        FK[k, x, ri] = (value * scale).astype(BF16)
        mine = FK.at[k, x, ri]
        for dy, dz in plane:
            send(("vp",), mine, mine, dev(dy=dy, dz=dz), out=CHUNKS + 3)

    def weight_4():
        wait_bytes(LIKE, rsem.at[groups[("vp",)]])
        mine = FK.at[k, x]
        for n in (2, 1, 3):
            send(("vx",), mine, mine, dev(dx=n), out=CHUNKS + 4)

    def weight_5():
        wait_bytes(FK.at[0, pl.ds(0, 3)], rsem.at[groups[("vx",)]])
        send(("vk",), FK.at[k], FK.at[k], dev(dk=1), out=CHUNKS + 5)

    def weight_6():
        wait_bytes(FK.at[0], rsem.at[groups[("vk",)]])
        for yy in range(SIDE):
            for zz in range(SIDE):
                lanes = slice(zz * TILE, (zz + 1) * TILE)
                for kk in range(2):
                    for xx in range(SIDE):
                        first = kk * 256 + xx * 64 + yy * 16
                        WO[first : first + 16, lanes] = FK[kk, xx, yy * SIDE + zz, 0:16, :].astype(F32)
        for zz in range(SIDE):
            BO[:, zz * TILE : (zz + 1) * TILE] = jnp.sum(
                FK[0, 0, zz, 16:24, :].astype(F32), axis=0, keepdims=True
            )

    def offset(c, name):
        e = first_way(c)
        return {"far": 2, "relay": e, "near": -e, "mine": 0}[name]

    def group_way(name):
        return 1 if name in ("far", "mine") else -1

    def sum_of(c, h, a, b):
        dy, dz = (a, b) if h == 0 else (b, a)
        column = (((y + dy + SIDE) % SIDE) * SIDE + (z + dz + SIDE) % SIDE) * 2 + h
        return Z[c][TS[8 + 3, column]]

    NAMES = ("far", "relay", "near", "mine")

    def back_0(c, i):
        name = NAMES[i]
        a, e = offset(c, name), group_way(name)
        for h in range(2):
            SB[c, h, i, 0] = sum_of(c, h, a, 2).astype(BF16)
            send(("bf", c, i), SB.at[c, h, i, 0], SR.at[c, h, i, 0], along(h, False, e))
        for h in range(2):
            SB[c, h, i, 1] = sum_of(c, h, a, -e).astype(BF16)
            send(("bd", c, i), SB.at[c, h, i, 1], SR.at[c, h, i, 1], along(h, False, -e))

    def back_1(c, i):
        name = NAMES[i]
        a, e = offset(c, name), group_way(name)
        take(("bf", c, i), 2)
        for h in range(2):
            SB[c, h, i, 2] = (sum_of(c, h, a, e) + SR[c, h, i, 0].astype(F32)).astype(BF16)
            send(("br", c, i), SB.at[c, h, i, 2], SR.at[c, h, i, 2], along(h, False, e))

    def back_2(c, i):
        name = NAMES[i]
        e = first_way(c)
        take(("bd", c, i), 2)
        take(("br", c, i), 2)
        if name == "relay":
            take(("tf", c), 2)
        for h in range(2):
            value = sum_of(c, h, offset(c, name), 0) + SR[c, h, i, 1].astype(F32)
            value = value + SR[c, h, i, 2].astype(F32)
            if name == "far":
                SB[c, h, 4, 0] = value.astype(BF16)
                send(("tf", c), SB.at[c, h, 4, 0], SR.at[c, h, 4, 0], along(h, True, e))
            elif name == "near":
                SB[c, h, 4, 1] = value.astype(BF16)
                send(("td", c), SB.at[c, h, 4, 1], SR.at[c, h, 4, 1], along(h, True, -e))
            elif name == "relay":
                SB[c, h, 4, 2] = (value + SR[c, h, 4, 0].astype(F32)).astype(BF16)
                send(("tr", c), SB.at[c, h, 4, 2], SR.at[c, h, 4, 2], along(h, True, e))
            else:
                UK[c, h] = value

    def back_3(c):
        take(("td", c), 2)
        take(("tr", c), 2)
        for h in range(2):
            value = UK[c, h] + SR[c, h, 4, 1].astype(F32)
            value = value + SR[c, h, 4, 2].astype(F32)
            FO[h * TILE : (h + 1) * TILE, c * WIDE : (c + 1) * WIDE] = value.astype(BF16)

    def multiply_back_all(c):
        spread_3(c)
        for part in range(3):
            multiply_back(c, part)

    steps = dict(w0=weight_0, w1=weight_1, w2=weight_2, w3=weight_3, w4=weight_4, w5=weight_5)
    steps.update(w6=weight_6, s0=spread_0, s1=spread_1, s2=spread_2, mm=multiply_back_all)
    steps.update(b0=back_0, b1=back_1, b2=back_2, b3=back_3)
    run(BACKWARD, steps)

    assert len(groups) == GROUPS, len(groups)
    for c in range(CHUNKS):
        wait_bytes(Z[c].at[pl.ds(0, 44)], ssem.at[c])
    for number, like in enumerate(
        (AK, PR, XB, LIKE, FK.at[0, pl.ds(0, 3)], FK.at[0]), start=CHUNKS
    ):
        wait_bytes(like, ssem.at[number])


def finish_kernel(a, b, c, d, ao, bo, co, do, sem):
    pairs = ((c, co), (a, ao), (b, bo), (d, do))
    copies = [pltpu.make_async_copy(p[0], p[1], sem.at[n]) for n, p in enumerate(pairs)]
    for copy in copies:
        copy.start()
    for copy in copies:
        copy.wait()


def shards(features, blocks, block_rows, block_cols, block_count, weight, bias_vector, upstream):
    scale = 1.0 / math.sqrt(features.shape[0] * SIDE * SIDE * SIDE * 2)
    vmem = pl.BlockSpec(memory_space=pltpu.VMEM)
    hbm = pl.BlockSpec(memory_space=pltpu.HBM)
    smem = pl.BlockSpec(memory_space=pltpu.SMEM)
    shapes = (
        jax.ShapeDtypeStruct((256, 512), BF16),
        jax.ShapeDtypeStruct((256, 512), BF16),
        jax.ShapeDtypeStruct((512, 512), F32),
        jax.ShapeDtypeStruct((1, 512), F32),
    )
    results = pl.pallas_call(
        functools.partial(step_kernel, scale),
        out_shape=shapes,
        in_specs=[smem] + [hbm] * 7,
        out_specs=(vmem, vmem, vmem, vmem),
        scratch_shapes=[
            *[pltpu.VMEM((KBLOCKS, TILE, WIDE), BF16)] * CHUNKS,
            *[pltpu.VMEM((SLOTS + 1, TILE, WIDE), F32)] * CHUNKS,
            *[pltpu.VMEM((IBLOCKS, TILE, WIDE), BF16)] * CHUNKS,
            pltpu.VMEM((SLOTS, TILE, TILE), BF16),
            pltpu.VMEM((SLOTS, TILE, TILE), BF16),
            pltpu.VMEM((512, 512), BF16),
            pltpu.VMEM((256, 512), BF16),
            pltpu.VMEM((CHUNKS, SIDE, 256, WIDE), BF16),
            pltpu.VMEM((CHUNKS, SIDE, 256, WIDE), BF16),
            pltpu.VMEM((CHUNKS, 3, 256, WIDE), BF16),
            pltpu.VMEM((CHUNKS, 3, 256, WIDE), BF16),
            pltpu.VMEM((256, 512), BF16),
            pltpu.VMEM((256, 512), BF16),
            pltpu.VMEM((CHUNKS, 2, TILE, WIDE), F32),
            pltpu.VMEM((CHUNKS, 2, 5, 3, TILE, WIDE), BF16),
            pltpu.VMEM((CHUNKS, 2, 5, 3, TILE, WIDE), BF16),
            pltpu.VMEM((2, 16, SIDE, 24, TILE), F32),
            pltpu.VMEM((16, SIDE, 24, TILE), F32),
            pltpu.VMEM((16, SIDE, 24, TILE), BF16),
            pltpu.VMEM((15, SIDE, 24, TILE), BF16),
            pltpu.VMEM((SIDE, 24, TILE), F32),
            pltpu.VMEM((3, 24, TILE), F32),
            pltpu.VMEM((2, SIDE, 16, 24, TILE), BF16),
            pltpu.VMEM((15, 24, TILE), BF16),
            pltpu.VMEM((1, SLOTS), jnp.int32),
            pltpu.VMEM((1, SLOTS), jnp.int32),
            pltpu.VMEM((1, 512), F32),
            pltpu.VMEM((16, TILE), jnp.int32),
            pltpu.VMEM((16, TILE), jnp.int32),
            pltpu.SMEM((16, TILE), jnp.int32),
            pltpu.SemaphoreType.DMA((LOCAL + 1,)),
            pltpu.SemaphoreType.DMA((CHUNKS + 6,)),
            pltpu.SemaphoreType.DMA((GROUPS,)),
        ],
        compiler_params=pltpu.CompilerParams(
            collective_id=0, has_side_effects=True, vmem_limit_bytes=46 * 2**20
        ),
        name="graph_layer",
    )(
        block_count,
        *[
            pltpu.with_memory_space_constraint(array, pltpu.HBM)
            for array in (
                block_rows[0],
                block_cols[0],
                features,
                blocks[0, 0],
                weight,
                bias_vector.reshape(1, 512),
                upstream,
            )
        ],
    )
    activated, grad_features, grad_weight, grad_bias = pl.pallas_call(
        finish_kernel,
        out_shape=shapes,
        in_specs=[vmem] * 4,
        out_specs=(hbm,) * 4,
        scratch_shapes=[pltpu.SemaphoreType.DMA((4,))],
        compiler_params=pltpu.CompilerParams(vmem_limit_bytes=2 * 2**20),
        name="finish",
    )(*results)
    return (activated, grad_weight, grad_bias.reshape(512), grad_features)


def solution(mesh):
    in_specs = (
        P(("col", "row"), None),
        P("row", "col", None, None, None),
        P("row", "col", None),
        P("row", "col", None),
        P("row", "col"),
        P(),
        P(),
        P(("row", "col"), None),
    )
    out_specs = (P(("row", "col"), None), P(), P(), P(("col", "row"), None))
    return jax.shard_map(shards, mesh=mesh, in_specs=in_specs, out_specs=out_specs, check_vma=False)
```

```python
import functools
import math

import jax
import jax.numpy as jnp
from jax import lax
from jax.experimental import pallas as pl
from jax.experimental.pallas import tpu as pltpu
from jax.sharding import PartitionSpec as P

MESH = pl.DeviceIdType.MESH
F32 = jnp.float32
BF16 = jnp.bfloat16
SIDE = 4
TILE = 128
WIDTHS = (256, 128, 128)
STARTS = (0, 256, 384)
CHUNKS = len(WIDTHS)
DIRECT_SUMS = (1, 2)
DIRECT_SPREAD = (1, 2)
HALF = 256
KBLOCKS = 32
IBLOCKS = 16
SLOTS = 48
SLOTS_AT_ONCE = 16
LOCAL = 2 * CHUNKS + 6
FORWARD = (
    ("g0", 0),
    ("g0", 2),
    ("own", 0),
    ("prep",),
    ("g1", 0),
    ("g0", 1),
    ("turn", 1),
    ("turn", 2),
    ("g3", 0),
    ("g1", 2),
    ("g2", 0),
    ("g4", 0),
    ("g6", 0),
    ("own", 2),
    ("g3", 2),
    ("g1", 1),
    ("g4", 2),
    ("mm", 0),
    ("g6", 2),
    ("own", 1),
    ("g2", 2),
    ("g3", 1),
    ("g4", 1),
    ("r1", 0),
    ("mm", 2),
    ("g2", 1),
    ("r2", 2),
    ("g6", 1),
    ("r2", 0),
    ("r1", 2),
    ("mm", 1),
    ("r1", 1),
    ("r3", 0),
    ("r2", 1),
    ("r3", 2),
    ("r3", 1),
)
BACKWARD = (
    ("s0", 1),
    ("w0",),
    ("s0", 2),
    ("s0", 0),
    ("s2", 1),
    ("w1",),
    ("s1", 1),
    ("s2", 2),
    ("mm", 1),
    ("s1", 2),
    ("b0", 1, 0),
    ("b0", 1, 3),
    ("b0", 1, 2),
    ("b0", 1, 1),
    ("s1", 0),
    ("mm", 2),
    ("b0", 2, 3),
    ("w2",),
    ("b0", 2, 1),
    ("b0", 2, 0),
    ("b1", 1, 2),
    ("b0", 2, 2),
    ("b1", 1, 3),
    ("s2", 0),
    ("b1", 1, 0),
    ("w3",),
    ("b1", 1, 1),
    ("mm", 0),
    ("b0", 0, 0),
    ("b0", 0, 2),
    ("b0", 0, 1),
    ("b1", 2, 1),
    ("w4",),
    ("b1", 0, 0),
    ("b2", 1, 0),
    ("b1", 2, 2),
    ("b1", 2, 0),
    ("b2", 1, 2),
    ("b1", 0, 2),
    ("b1", 0, 1),
    ("b0", 0, 3),
    ("b2", 0, 0),
    ("b1", 2, 3),
    ("b2", 2, 0),
    ("b2", 1, 3),
    ("w5",),
    ("b2", 2, 2),
    ("b2", 1, 1),
    ("b1", 0, 3),
    ("b2", 0, 2),
    ("b2", 0, 1),
    ("b2", 2, 1),
    ("b2", 2, 3),
    ("b3", 1),
    ("b2", 0, 3),
    ("w6",),
    ("b3", 0),
    ("b3", 2),
)
FAR = 1 << 17
GROUPS = 41 * CHUNKS + 6 - len(DIRECT_SUMS) - len(DIRECT_SPREAD)


def wrap(value):
    return value % SIDE


def at_k(h, a, b):
    a, b = wrap(a), wrap(b)
    dy, dz = (a, b) if h == 0 else (b, a)
    return (dy * SIDE + dz) * 2 + h


def step_kernel(scale, count, rows_in, cols_in, feat, blocks, weight, bias, ups, *refs):
    AO, FO, WO, BO = refs[:4]
    refs = refs[4:]
    by_chunk = [refs[n * CHUNKS : (n + 1) * CHUNKS] for n in range(10)]
    G, Z, DG, S1, R0, XS, XR, UK, SB, SR = by_chunk
    refs = refs[10 * CHUNKS :]
    BK, BT, WT, UP, HD, DP = refs[:6]
    GP, AK, PX, PR, XA, XB, FK, LIKE = refs[6:14]
    RV, CV, BV, IX, TV, TS, lsem, ssem, rsem = refs[14:]
    ri = lax.axis_index("row")
    ci = lax.axis_index("col")
    y, z = ri // SIDE, ri % SIDE
    x, k = ci // 2, ci % 2
    turn = 1 - 2 * k

    def dev(dy=0, dz=0, dx=0, dk=0):
        row = ((y + dy + SIDE) % SIDE) * SIDE + (z + dz + SIDE) % SIDE
        col = ((x + dx + SIDE) % SIDE) * 2 + (k + dk) % 2
        return (row, col)

    def along(h, first, step):
        if (h == 0) == first:
            return dev(dy=step)
        return dev(dz=step)

    groups = {}

    def send(group, src, dst, to, out=None):
        number = groups.setdefault(group, len(groups))
        pltpu.make_async_remote_copy(
            src_ref=src,
            dst_ref=dst,
            send_sem=ssem.at[group[1] if out is None else out],
            recv_sem=rsem.at[number],
            device_id=to,
            device_id_type=MESH,
        ).start()

    def wait_bytes(like, sem):
        pltpu.make_async_copy(like, like, sem).wait()

    def take(group, units):
        wait_bytes(G[group[1]].at[pl.ds(0, units)], rsem.at[groups[group]])

    local = []

    def fetch(src, dst):
        copy = pltpu.make_async_copy(src, dst, lsem.at[len(local)])
        copy.start()
        local.append(copy)
        return copy

    own = [
        [
            fetch(
                feat.at[pl.ds(h * TILE, TILE), pl.ds(STARTS[c], WIDTHS[c])],
                G[c].at[at_k(h, 0, 0)],
            )
            for h in range(2)
        ]
        for c in range(CHUNKS)
    ]
    blocks_in = fetch(blocks, BK)
    weight_in = fetch(weight, WT)
    rows_got = fetch(rows_in, RV)
    cols_got = fetch(cols_in, CV)
    ups_in = fetch(ups, UP)
    bias_in = fetch(bias, BV)

    barrier = pltpu.get_barrier_semaphore()
    partners = [dev(dk=1)]
    for step in (1, -1):
        partners += [dev(dy=step), dev(dz=step), dev(dx=step)]
    for partner in partners:
        pl.semaphore_signal(barrier, inc=1, device_id=partner, device_id_type=MESH)
    for c in range(CHUNKS):
        Z[c][SLOTS] = jnp.zeros((TILE, WIDTHS[c]), F32)
    IX[...] = jnp.zeros_like(IX)
    pl.semaphore_wait(barrier, len(partners))

    def first_way(c):
        return (1, -1, -1)[c]

    def second_way(a):
        return 1 if a in (0, 1) else -1

    def second_sends(c, a):
        for h in range(2):
            src = G[c].at[at_k(h, a, 0)]
            for step in (1, -1):
                side = "in" if step == second_way(a) else "by"
                name = "all" if side == "by" and a in (1, -1) else a
                send(
                    ("g2" + side, c, name),
                    src,
                    G[c].at[at_k(h, a, -step)],
                    along(h, False, step),
                )

    def gather_0(c):
        for h in range(2):
            own[c][h].wait()
            src = G[c].at[at_k(h, 0, 0)]
            for step in (first_way(c), -first_way(c)):
                side = "in" if step == first_way(c) else "by"
                send(("g1" + side, c), src, G[c].at[at_k(h, -step, 0)], along(h, True, step))

    def gather_own(c):
        second_sends(c, 0)

    def gather_1(c):
        e = first_way(c)
        take(("g1in", c), 2)
        for h in range(2):
            send(
                ("g1r", c),
                G[c].at[at_k(h, -e, 0)],
                G[c].at[at_k(h, 2, 0)],
                along(h, True, e),
            )
        second_sends(c, -e)
        take(("g1by", c), 2)
        second_sends(c, e)

    def second_relay(c, a):
        e = second_way(a)
        take(("g2in", c, a), 2)
        for h in range(2):
            send(
                ("g2r", c, "all" if a in (1, -1) else a),
                G[c].at[at_k(h, a, -e)],
                G[c].at[at_k(h, a, 2)],
                along(h, False, e),
            )

    def gather_2(c):
        second_relay(c, 0)

    def gather_3(c):
        take(("g1r", c), 2)
        second_sends(c, 2)

    def gather_4(c):
        second_relay(c, first_way(c) * -1)
        second_relay(c, first_way(c))

    def gather_6(c):
        second_relay(c, 2)

    def gather_8(c):
        take(("g2by", c, 0), 2)
        take(("g2by", c, "all"), 4)
        take(("g2by", c, 2), 2)
        take(("g2r", c, 0), 2)
        take(("g2r", c, "all"), 4)
        take(("g2r", c, 2), 2)

    def tables_0():
        rows_got.wait()
        cols_got.wait()
        IX[0:1, 0:SLOTS] = RV[...]
        IX[8:9, 0:SLOTS] = CV[...]
        lane = lax.broadcasted_iota(jnp.int32, (TILE, TILE), 1)
        down = lax.broadcasted_iota(jnp.int32, (TILE, TILE), 0)
        rows = jnp.broadcast_to(IX[0:1, :], (TILE, TILE))
        cols = jnp.broadcast_to(IX[8:9, :], (TILE, TILE))
        live = lane < count[0, 0]
        for which, key in enumerate((rows * KBLOCKS + cols, cols * IBLOCKS + rows)):
            shift = 5 if which == 0 else 4
            key = jnp.where(live, key, FAR + lane)
            key_down = key.T
            own, other = key_down >> shift, key_down & ((1 << shift) - 1)
            less = key < key_down
            rank = jnp.sum(jnp.where(less, 1, 0), axis=1, keepdims=True)
            same = less & ((key >> shift) == own)
            keep = jnp.minimum(jnp.sum(jnp.where(same, 1, 0), axis=1, keepdims=True), 1)
            if which == 0:
                piece = other >> 1
                dy = ((piece >> 2) + SIDE - y) & 3
                dz = (piece + SIDE - z) & 3
                place = (dy * SIDE + dz) * 2 + (other & 1)
            else:
                to_col = other >> 1
                dx = (turn * ((to_col >> 1) - x)) & 3
                dk = (to_col + 2 - k) & 1
                place = (dk * SIDE + dx) * 2 + (other & 1)
            hit = rank == lane
            upto = jnp.sum(jnp.where(own <= lane, 1, 0), axis=0, keepdims=True)
            any_own = jnp.sum(jnp.where(own == lane, 1, 0), axis=0, keepdims=True)
            at = which * 8
            TV[at : at + 1, :] = jnp.sum(jnp.where(hit, down, 0), axis=0, keepdims=True)
            TV[at + 1 : at + 2, :] = jnp.sum(jnp.where(hit, place, 0), axis=0, keepdims=True)
            TV[at + 2 : at + 3, :] = jnp.sum(jnp.where(hit, keep, 0), axis=0, keepdims=True)
            TV[at + 3 : at + 4, :] = jnp.where(any_own > 0, upto - 1, SLOTS)

    def tables_1():
        copy = pltpu.make_async_copy(TV, TS, lsem.at[LOCAL])
        copy.start()
        copy.wait()

    def product(c, which, part):
        at = which * 8
        base = part * SLOTS_AT_ONCE
        total = None if part == 0 else Z[c][base - 1]
        for slot in range(base, base + SLOTS_AT_ONCE):
            place = TS[at + 1, slot]
            block = (BK if which == 0 else BT)[TS[at, slot]]
            value = jnp.dot(block, (G if which == 0 else DG)[c][place], preferred_element_type=F32)
            if total is not None:
                value = value + total * TS[at + 2, slot].astype(F32)
            Z[c][slot] = value
            total = value

    def multiply(c, part):
        product(c, 0, part)

    def multiply_back(c, part):
        product(c, 1, part)

    def part_of(c, dk, dx):
        row = (((x + turn * dx + SIDE) % SIDE) * 2 + (k + dk) % 2) * 2
        return jnp.concatenate([Z[c][TS[3, row]], Z[c][TS[3, row + 1]]], axis=0)

    def reduce_0(c):
        for dx in (2, 3, 1, 0):
            S1[c][dx] = part_of(c, 1, dx).astype(BF16)
            mirrored = wrap(-dx)
            send(("c0", c, mirrored), S1[c].at[dx], R0[c].at[mirrored], dev(dk=1))

    def paired(c, dx):
        take(("c0", c, dx), 2)
        return part_of(c, 0, dx) + R0[c][dx].astype(F32)

    def reduce_1(c):
        XS[c][0] = paired(c, 2).astype(BF16)
        if c in DIRECT_SUMS:
            send(("cf", c), XS[c].at[0], XR[c].at[0], dev(dx=2))
        else:
            for half in range(2):
                lines = pl.ds(half * TILE, TILE)
                send(("cf", c, half), XS[c].at[0, lines], XR[c].at[0, lines], dev(dx=turn))
        XS[c][1] = paired(c, 3).astype(BF16)
        send(("cd", c), XS[c].at[1], XR[c].at[1], dev(dx=-turn))
        if c in DIRECT_SUMS:
            XS[c][2] = paired(c, 1).astype(BF16)
            send(("cr", c), XS[c].at[2], XR[c].at[2], dev(dx=turn))

    def reduce_2(c):
        if c in DIRECT_SUMS:
            return
        value = paired(c, 1)
        for half in range(2):
            lines = pl.ds(half * TILE, TILE)
            part = value[half * TILE : (half + 1) * TILE]
            take(("cf", c, half), 1)
            XS[c][2, lines] = (part + XR[c][0, lines].astype(F32)).astype(BF16)
            send(("cr", c), XS[c].at[2, lines], XR[c].at[2, lines], dev(dx=turn))

    def reduce_3(c):
        value = paired(c, 0)
        take(("cd", c), 2)
        value = value + XR[c][1].astype(F32)
        take(("cr", c), 2)
        value = value + XR[c][2].astype(F32)
        if c in DIRECT_SUMS:
            take(("cf", c), 2)
            value = value + XR[c][0].astype(F32)
        HD[:, STARTS[c] : STARTS[c] + WIDTHS[c]] = value.astype(BF16)

    def turn_blocks(part):
        @pl.loop(0, SLOTS_AT_ONCE // 4)
        def _(n):
            for j in range(4):
                s = part * SLOTS_AT_ONCE + n * 4 + j
                BT[s] = BK[s].T

    def run(order, table):
        for name, *args in order:
            table[name](*args)

    def prepare():
        tables_0()
        blocks_in.wait()
        turn_blocks(0)
        tables_1()

    def multiply_all(c):
        gather_8(c)
        for part in range(3):
            multiply(c, part)
        reduce_0(c)

    steps = dict(g0=gather_0, own=gather_own, g1=gather_1, g2=gather_2, g3=gather_3, g4=gather_4)
    steps.update(g6=gather_6, mm=multiply_all, r1=reduce_1, r2=reduce_2, r3=reduce_3)
    steps.update(prep=prepare, turn=turn_blocks)
    run(FORWARD, steps)
    weight_in.wait()
    ups_in.wait()

    bias_rows = []
    bias_in.wait()
    for n in range(2):
        columns = slice(n * HALF, (n + 1) * HALF)
        pre = jnp.dot(HD[...], WT[:, columns], preferred_element_type=F32) + BV[:, columns]
        sig = jax.nn.sigmoid(pre)
        AO[:, columns] = (pre * sig).astype(BF16)
        dpre = (UP[:, columns].astype(F32) * sig * (1.0 + pre * (1.0 - sig))).astype(BF16)
        DP[:, columns] = dpre
        bias_rows.append(jnp.sum(dpre.astype(F32).reshape(32, 8, HALF), axis=0))

    def hidden(c, place):
        return DG[c].at[pl.ds(2 * place, 2)]

    def spread_0(c):
        value = lax.dot_general(
            DP[...],
            WT[pl.ds(STARTS[c], WIDTHS[c]), :],
            (((1,), (1,)), ((), ())),
            preferred_element_type=F32,
        )
        DG[c][0:2] = value.astype(BF16).reshape(2, TILE, WIDTHS[c])
        if c in DIRECT_SPREAD:
            send(("sr", c), hidden(c, 0), hidden(c, 2), dev(dx=2))
            send(("sp", c), hidden(c, 0), hidden(c, 3), dev(dx=turn))
        else:
            for half in range(2):
                send(("sp", c, half), DG[c].at[half], DG[c].at[6 + half], dev(dx=turn))
        send(("sm", c), hidden(c, 0), hidden(c, 1), dev(dx=-turn))
        send(("sc", c), hidden(c, 0), hidden(c, SIDE), dev(dk=1))

    def spread_1(c):
        if c in DIRECT_SPREAD:
            take(("sp", c), 2)
        else:
            for half in range(2):
                take(("sp", c, half), 1)
                send(("sr", c), DG[c].at[6 + half], DG[c].at[4 + half], dev(dx=turn))
        send(("sc", c), hidden(c, 3), hidden(c, SIDE + 1), dev(dk=1))
        take(("sm", c), 2)
        send(("sc", c), hidden(c, 1), hidden(c, SIDE + 3), dev(dk=1))

    def spread_2(c):
        take(("sr", c), 2)
        send(("sc", c), hidden(c, 2), hidden(c, SIDE + 2), dev(dk=1))

    def spread_3(c):
        take(("sc", c), 8)

    plane = [(dy, dz) for dy in range(SIDE) for dz in range(SIDE) if dy or dz]

    def weight_0():
        value = lax.dot_general(
            HD[...], DP[...], (((0,), (0,)), ((), ())), preferred_element_type=F32
        )
        for zz in range(SIDE):
            lanes = slice(zz * TILE, (zz + 1) * TILE)
            tiles = value[:, lanes].reshape(2, SIDE, SIDE, 16, TILE)
            sums = bias_rows[zz // 2][:, (zz % 2) * TILE : (zz % 2 + 1) * TILE]
            for yy in range(SIDE):
                GP[:, yy * SIDE + zz, :, 0:16, :] = tiles[:, :, yy]
                GP[:, yy * SIDE + zz, :, 16:24, :] = jnp.broadcast_to(
                    sums, (2, SIDE, 8, TILE)
                )
        send(("wk",), GP.at[1 - k], AK, dev(dk=1), out=CHUNKS + 0)

    def weight_1():
        wait_bytes(AK, rsem.at[groups[("wk",)]])
        AK[...] = GP[k] + AK[...]
        PX[...] = AK[...].astype(BF16)
        for n, (dy, dz) in enumerate(plane):
            there = ((y + dy) % SIDE) * SIDE + (z + dz) % SIDE
            send(("wp",), PX.at[there], PR.at[n], dev(dy=dy, dz=dz), out=CHUNKS + 1)

    def weight_2():
        wait_bytes(PR, rsem.at[groups[("wp",)]])
        value = AK[ri]
        for n in range(len(plane)):
            value = value + PR[n].astype(F32)
        XA[...] = value
        for n in (2, 1, 3):
            send(("wx",), XA.at[(x + n) % SIDE], XB.at[n - 1], dev(dx=n), out=CHUNKS + 2)

    def weight_3():
        wait_bytes(XB, rsem.at[groups[("wx",)]])
        value = XA[x]
        for n in range(3):
            value = value + XB[n]
        FK[k, x, ri] = (value * scale).astype(BF16)
        mine = FK.at[k, x, ri]
        for dy, dz in plane:
            send(("vp",), mine, mine, dev(dy=dy, dz=dz), out=CHUNKS + 3)

    def weight_4():
        wait_bytes(LIKE, rsem.at[groups[("vp",)]])
        mine = FK.at[k, x]
        for n in (2, 1, 3):
            send(("vx",), mine, mine, dev(dx=n), out=CHUNKS + 4)

    def weight_5():
        wait_bytes(FK.at[0, pl.ds(0, 3)], rsem.at[groups[("vx",)]])
        send(("vk",), FK.at[k], FK.at[k], dev(dk=1), out=CHUNKS + 5)

    def weight_6():
        wait_bytes(FK.at[0], rsem.at[groups[("vk",)]])
        for yy in range(SIDE):
            for zz in range(SIDE):
                lanes = slice(zz * TILE, (zz + 1) * TILE)
                for kk in range(2):
                    for xx in range(SIDE):
                        first = kk * 256 + xx * 64 + yy * 16
                        WO[first : first + 16, lanes] = FK[kk, xx, yy * SIDE + zz, 0:16, :].astype(F32)
        for zz in range(SIDE):
            BO[:, zz * TILE : (zz + 1) * TILE] = jnp.sum(
                FK[0, 0, zz, 16:24, :].astype(F32), axis=0, keepdims=True
            )

    def offset(c, name):
        e = first_way(c)
        return {"far": 2, "relay": e, "near": -e, "mine": 0}[name]

    def group_way(name):
        return 1 if name in ("far", "mine") else -1

    def sum_of(c, h, a, b):
        dy, dz = (a, b) if h == 0 else (b, a)
        column = (((y + dy + SIDE) % SIDE) * SIDE + (z + dz + SIDE) % SIDE) * 2 + h
        return Z[c][TS[8 + 3, column]]

    NAMES = ("far", "relay", "near", "mine")

    def back_0(c, i):
        name = NAMES[i]
        a, e = offset(c, name), group_way(name)
        for h in range(2):
            SB[c][h, i, 0] = sum_of(c, h, a, 2).astype(BF16)
            send(("bf", c, i), SB[c].at[h, i, 0], SR[c].at[h, i, 0], along(h, False, e))
        for h in range(2):
            SB[c][h, i, 1] = sum_of(c, h, a, -e).astype(BF16)
            send(("bd", c, i), SB[c].at[h, i, 1], SR[c].at[h, i, 1], along(h, False, -e))

    def back_1(c, i):
        name = NAMES[i]
        a, e = offset(c, name), group_way(name)
        take(("bf", c, i), 2)
        for h in range(2):
            SB[c][h, i, 2] = (sum_of(c, h, a, e) + SR[c][h, i, 0].astype(F32)).astype(BF16)
            send(("br", c, i), SB[c].at[h, i, 2], SR[c].at[h, i, 2], along(h, False, e))

    def back_2(c, i):
        name = NAMES[i]
        e = first_way(c)
        take(("bd", c, i), 2)
        take(("br", c, i), 2)
        if name == "relay":
            take(("tf", c), 2)
        for h in range(2):
            value = sum_of(c, h, offset(c, name), 0) + SR[c][h, i, 1].astype(F32)
            value = value + SR[c][h, i, 2].astype(F32)
            if name == "far":
                SB[c][h, 4, 0] = value.astype(BF16)
                send(("tf", c), SB[c].at[h, 4, 0], SR[c].at[h, 4, 0], along(h, True, e))
            elif name == "near":
                SB[c][h, 4, 1] = value.astype(BF16)
                send(("td", c), SB[c].at[h, 4, 1], SR[c].at[h, 4, 1], along(h, True, -e))
            elif name == "relay":
                SB[c][h, 4, 2] = (value + SR[c][h, 4, 0].astype(F32)).astype(BF16)
                send(("tr", c), SB[c].at[h, 4, 2], SR[c].at[h, 4, 2], along(h, True, e))
            else:
                UK[c][h] = value

    def back_3(c):
        take(("td", c), 2)
        take(("tr", c), 2)
        for h in range(2):
            value = UK[c][h] + SR[c][h, 4, 1].astype(F32)
            value = value + SR[c][h, 4, 2].astype(F32)
            FO[h * TILE : (h + 1) * TILE, STARTS[c] : STARTS[c] + WIDTHS[c]] = value.astype(BF16)

    def multiply_back_all(c):
        spread_3(c)
        for part in range(3):
            multiply_back(c, part)

    steps = dict(w0=weight_0, w1=weight_1, w2=weight_2, w3=weight_3, w4=weight_4, w5=weight_5)
    steps.update(w6=weight_6, s0=spread_0, s1=spread_1, s2=spread_2, mm=multiply_back_all)
    steps.update(b0=back_0, b1=back_1, b2=back_2, b3=back_3)
    run(BACKWARD, steps)

    assert len(groups) == GROUPS, len(groups)
    for c in range(CHUNKS):
        wait_bytes(Z[c].at[pl.ds(0, 44)], ssem.at[c])
    for number, like in enumerate(
        (AK, PR, XB, LIKE, FK.at[0, pl.ds(0, 3)], FK.at[0]), start=CHUNKS
    ):
        wait_bytes(like, ssem.at[number])


def finish_kernel(a, b, c, d, ao, bo, co, do, sem):
    pairs = ((c, co), (a, ao), (b, bo), (d, do))
    copies = [pltpu.make_async_copy(p[0], p[1], sem.at[n]) for n, p in enumerate(pairs)]
    for copy in copies:
        copy.start()
    for copy in copies:
        copy.wait()


def shards(features, blocks, block_rows, block_cols, block_count, weight, bias_vector, upstream):
    scale = 1.0 / math.sqrt(features.shape[0] * SIDE * SIDE * SIDE * 2)
    vmem = pl.BlockSpec(memory_space=pltpu.VMEM)
    hbm = pl.BlockSpec(memory_space=pltpu.HBM)
    smem = pl.BlockSpec(memory_space=pltpu.SMEM)
    shapes = (
        jax.ShapeDtypeStruct((256, 512), BF16),
        jax.ShapeDtypeStruct((256, 512), BF16),
        jax.ShapeDtypeStruct((512, 512), F32),
        jax.ShapeDtypeStruct((1, 512), F32),
    )
    results = pl.pallas_call(
        functools.partial(step_kernel, scale),
        out_shape=shapes,
        in_specs=[smem] + [hbm] * 7,
        out_specs=(vmem, vmem, vmem, vmem),
        scratch_shapes=[
            *[pltpu.VMEM((KBLOCKS, TILE, w), BF16) for w in WIDTHS],
            *[pltpu.VMEM((SLOTS + 1, TILE, w), F32) for w in WIDTHS],
            *[pltpu.VMEM((IBLOCKS, TILE, w), BF16) for w in WIDTHS],
            *[pltpu.VMEM((SIDE, 256, w), BF16) for w in WIDTHS],
            *[pltpu.VMEM((SIDE, 256, w), BF16) for w in WIDTHS],
            *[pltpu.VMEM((3, 256, w), BF16) for w in WIDTHS],
            *[pltpu.VMEM((3, 256, w), BF16) for w in WIDTHS],
            *[pltpu.VMEM((2, TILE, w), F32) for w in WIDTHS],
            *[pltpu.VMEM((2, 5, 3, TILE, w), BF16) for w in WIDTHS],
            *[pltpu.VMEM((2, 5, 3, TILE, w), BF16) for w in WIDTHS],
            pltpu.VMEM((SLOTS, TILE, TILE), BF16),
            pltpu.VMEM((SLOTS, TILE, TILE), BF16),
            pltpu.VMEM((512, 512), BF16),
            pltpu.VMEM((256, 512), BF16),
            pltpu.VMEM((256, 512), BF16),
            pltpu.VMEM((256, 512), BF16),
            pltpu.VMEM((2, 16, SIDE, 24, TILE), F32),
            pltpu.VMEM((16, SIDE, 24, TILE), F32),
            pltpu.VMEM((16, SIDE, 24, TILE), BF16),
            pltpu.VMEM((15, SIDE, 24, TILE), BF16),
            pltpu.VMEM((SIDE, 24, TILE), F32),
            pltpu.VMEM((3, 24, TILE), F32),
            pltpu.VMEM((2, SIDE, 16, 24, TILE), BF16),
            pltpu.VMEM((15, 24, TILE), BF16),
            pltpu.VMEM((1, SLOTS), jnp.int32),
            pltpu.VMEM((1, SLOTS), jnp.int32),
            pltpu.VMEM((1, 512), F32),
            pltpu.VMEM((16, TILE), jnp.int32),
            pltpu.VMEM((16, TILE), jnp.int32),
            pltpu.SMEM((16, TILE), jnp.int32),
            pltpu.SemaphoreType.DMA((LOCAL + 1,)),
            pltpu.SemaphoreType.DMA((CHUNKS + 6,)),
            pltpu.SemaphoreType.DMA((GROUPS,)),
        ],
        compiler_params=pltpu.CompilerParams(
            collective_id=0, has_side_effects=True, vmem_limit_bytes=46 * 2**20
        ),
        name="graph_layer",
    )(
        block_count,
        *[
            pltpu.with_memory_space_constraint(array, pltpu.HBM)
            for array in (
                block_rows[0],
                block_cols[0],
                features,
                blocks[0, 0],
                weight,
                bias_vector.reshape(1, 512),
                upstream,
            )
        ],
    )
    activated, grad_features, grad_weight, grad_bias = pl.pallas_call(
        finish_kernel,
        out_shape=shapes,
        in_specs=[vmem] * 4,
        out_specs=(hbm,) * 4,
        scratch_shapes=[pltpu.SemaphoreType.DMA((4,))],
        compiler_params=pltpu.CompilerParams(vmem_limit_bytes=2 * 2**20),
        name="finish",
    )(*results)
    return (activated, grad_weight, grad_bias.reshape(512), grad_features)


def solution(mesh):
    in_specs = (
        P(("col", "row"), None),
        P("row", "col", None, None, None),
        P("row", "col", None),
        P("row", "col", None),
        P("row", "col"),
        P(),
        P(),
        P(("row", "col"), None),
    )
    out_specs = (P(("row", "col"), None), P(), P(), P(("col", "row"), None))
    return jax.shard_map(shards, mesh=mesh, in_specs=in_specs, out_specs=out_specs, check_vma=False)
```

```python
import functools
import math

import jax
import jax.numpy as jnp
from jax import lax
from jax.experimental import pallas as pl
from jax.experimental.pallas import tpu as pltpu
from jax.sharding import PartitionSpec as P

MESH = pl.DeviceIdType.MESH
F32 = jnp.float32
BF16 = jnp.bfloat16
SIDE = 4
TILE = 128
WIDTHS = (128, 128, 128, 128)
STARTS = (0, 128, 256, 384)
CHUNKS = len(WIDTHS)
DIRECT_SUMS = (2, 3)
DIRECT_SPREAD = (0, 1, 2, 3)
DIRECT_LAST = ()
HALF = 256
KBLOCKS = 32
IBLOCKS = 16
SLOTS = 48
SLOTS_AT_ONCE = 16
LOCAL = 2 * CHUNKS + 6
FORWARD = (
    ("g0", 0),
    ("g0", 1),
    ("own", 0),
    ("own", 1),
    ("prep",),
    ("g0", 2),
    ("g1", 0),
    ("g1", 1),
    ("g2", 0),
    ("turn", 1),
    ("g3", 0),
    ("g1", 2),
    ("g0", 3),
    ("g2", 1),
    ("turn", 2),
    ("g3", 1),
    ("g4", 0),
    ("own", 2),
    ("g6", 0),
    ("g4", 1),
    ("g3", 2),
    ("g6", 1),
    ("g1", 3),
    ("mm", 0),
    ("g6", 2),
    ("g2", 2),
    ("g4", 2),
    ("g3", 3),
    ("mm", 1),
    ("own", 3),
    ("g4", 3),
    ("r1", 0),
    ("mm", 2),
    ("r1", 1),
    ("g6", 3),
    ("g2", 3),
    ("r2", 0),
    ("r1", 2),
    ("mm", 3),
    ("r2", 1),
    ("r2", 2),
    ("r1", 3),
    ("r3", 1),
    ("r3", 0),
    ("r3", 2),
    ("r2", 3),
    ("r3", 3),
)
BACKWARD = (
    ("s0", 0),
    ("w0",),
    ("s0", 1),
    ("w1",),
    ("s2", 0),
    ("s1", 0),
    ("s0", 3),
    ("mm", 0),
    ("s2", 1),
    ("b0", 0, 3),
    ("s1", 1),
    ("b0", 0, 2),
    ("s0", 2),
    ("b0", 0, 1),
    ("b0", 0, 0),
    ("mm", 1),
    ("b0", 1, 2),
    ("s2", 3),
    ("b0", 1, 0),
    ("s1", 3),
    ("b0", 1, 1),
    ("b0", 1, 3),
    ("b1", 0, 2),
    ("w2",),
    ("mm", 3),
    ("s2", 2),
    ("b0", 3, 3),
    ("s1", 2),
    ("b1", 1, 2),
    ("b0", 3, 2),
    ("b0", 3, 0),
    ("b1", 1, 0),
    ("w3",),
    ("mm", 2),
    ("b0", 2, 0),
    ("b0", 2, 2),
    ("b0", 2, 1),
    ("b1", 3, 2),
    ("b0", 2, 3),
    ("b1", 0, 3),
    ("b1", 2, 0),
    ("b1", 0, 0),
    ("b2", 1, 0),
    ("b1", 3, 0),
    ("b0", 3, 1),
    ("b1", 2, 2),
    ("b1", 3, 3),
    ("w4",),
    ("b1", 2, 1),
    ("b1", 1, 3),
    ("b2", 0, 3),
    ("b1", 1, 1),
    ("b1", 0, 1),
    ("b2", 2, 0),
    ("b2", 3, 0),
    ("b2", 0, 0),
    ("b2", 1, 2),
    ("b1", 3, 1),
    ("b2", 0, 2),
    ("b2", 3, 2),
    ("b2", 2, 2),
    ("b1", 2, 3),
    ("b2", 1, 1),
    ("b2", 1, 3),
    ("b2", 2, 1),
    ("b2", 0, 1),
    ("b2", 3, 3),
    ("b2", 3, 1),
    ("w5",),
    ("b2", 2, 3),
    ("b3", 2),
    ("w6",),
    ("b3", 1),
    ("b3", 0),
    ("b3", 3),
)
FAR = 1 << 17
GROUPS = 30 * CHUNKS + 6 - 2 * len(DIRECT_SUMS) - len(DIRECT_SPREAD)


def wrap(value):
    return value % SIDE


def at_k(h, a, b):
    a, b = wrap(a), wrap(b)
    dy, dz = (a, b) if h == 0 else (b, a)
    return (dy * SIDE + dz) * 2 + h


def step_kernel(scale, count, rows_in, cols_in, feat, blocks, weight, bias, ups, *refs):
    AO, FO, WO, BO = refs[:4]
    refs = refs[4:]
    by_chunk = [refs[n * CHUNKS : (n + 1) * CHUNKS] for n in range(10)]
    G, Z, DG, S1, R0, XS, XR, UK, SB, SR = by_chunk
    refs = refs[10 * CHUNKS :]
    BK, BT, WT, UP, HD, DP = refs[:6]
    GP, AK, PX, PR, XA, XB, FK, LIKE = refs[6:14]
    RV, CV, BV, IX, TV, TS, lsem, ssem, rsem = refs[14:]
    ri = lax.axis_index("row")
    ci = lax.axis_index("col")
    y, z = ri // SIDE, ri % SIDE
    x, k = ci // 2, ci % 2
    turn = 1 - 2 * k

    def dev(dy=0, dz=0, dx=0, dk=0):
        row = ((y + dy + SIDE) % SIDE) * SIDE + (z + dz + SIDE) % SIDE
        col = ((x + dx + SIDE) % SIDE) * 2 + (k + dk) % 2
        return (row, col)

    def along(h, first, step):
        if (h == 0) == first:
            return dev(dy=step)
        return dev(dz=step)

    groups = {}

    def send(group, src, dst, to, out=None):
        number = groups.setdefault(group, len(groups))
        pltpu.make_async_remote_copy(
            src_ref=src,
            dst_ref=dst,
            send_sem=ssem.at[group[1] if out is None else out],
            recv_sem=rsem.at[number],
            device_id=to,
            device_id_type=MESH,
        ).start()

    def wait_bytes(like, sem):
        pltpu.make_async_copy(like, like, sem).wait()

    def take(group, units):
        wait_bytes(G[group[1]].at[pl.ds(0, units)], rsem.at[groups[group]])

    local = []

    def fetch(src, dst):
        copy = pltpu.make_async_copy(src, dst, lsem.at[len(local)])
        copy.start()
        local.append(copy)
        return copy

    own = [
        [
            fetch(
                feat.at[pl.ds(h * TILE, TILE), pl.ds(STARTS[c], WIDTHS[c])],
                G[c].at[at_k(h, 0, 0)],
            )
            for h in range(2)
        ]
        for c in range(CHUNKS)
    ]
    blocks_in = fetch(blocks, BK)
    weight_in = fetch(weight, WT)
    rows_got = fetch(rows_in, RV)
    cols_got = fetch(cols_in, CV)
    ups_in = fetch(ups, UP)
    bias_in = fetch(bias, BV)

    barrier = pltpu.get_barrier_semaphore()
    partners = [dev(dk=1)]
    for step in (1, -1):
        partners += [dev(dy=step), dev(dz=step), dev(dx=step)]
    for partner in partners:
        pl.semaphore_signal(barrier, inc=1, device_id=partner, device_id_type=MESH)
    for c in range(CHUNKS):
        Z[c][SLOTS] = jnp.zeros((TILE, WIDTHS[c]), F32)
    IX[...] = jnp.zeros_like(IX)
    pl.semaphore_wait(barrier, len(partners))

    def first_way(c):
        return (1, -1, 1, -1)[c]

    def second_way(a):
        return 1 if a in (0, 1) else -1

    def second_sends(c, a):
        for h in range(2):
            src = G[c].at[at_k(h, a, 0)]
            for step in (1, -1):
                send(
                    ("g2in", c, a) if step == second_way(a) else ("g2", c),
                    src,
                    G[c].at[at_k(h, a, -step)],
                    along(h, False, step),
                )

    def gather_0(c):
        for h in range(2):
            own[c][h].wait()
            src = G[c].at[at_k(h, 0, 0)]
            for step in (first_way(c), -first_way(c)):
                side = "in" if step == first_way(c) else "by"
                send(("g1" + side, c), src, G[c].at[at_k(h, -step, 0)], along(h, True, step))

    def gather_own(c):
        second_sends(c, 0)

    def gather_1(c):
        e = first_way(c)
        take(("g1in", c), 2)
        for h in range(2):
            send(
                ("g1r", c),
                G[c].at[at_k(h, -e, 0)],
                G[c].at[at_k(h, 2, 0)],
                along(h, True, e),
            )
        second_sends(c, -e)
        take(("g1by", c), 2)
        second_sends(c, e)

    def second_relay(c, a):
        e = second_way(a)
        take(("g2in", c, a), 2)
        for h in range(2):
            send(
                ("g2", c),
                G[c].at[at_k(h, a, -e)],
                G[c].at[at_k(h, a, 2)],
                along(h, False, e),
            )

    def gather_2(c):
        second_relay(c, 0)

    def gather_3(c):
        take(("g1r", c), 2)
        second_sends(c, 2)

    def gather_4(c):
        second_relay(c, first_way(c) * -1)
        second_relay(c, first_way(c))

    def gather_6(c):
        second_relay(c, 2)

    def gather_8(c):
        take(("g2", c), 16)

    def tables_0():
        rows_got.wait()
        cols_got.wait()
        IX[0:1, 0:SLOTS] = RV[...]
        IX[8:9, 0:SLOTS] = CV[...]
        lane = lax.broadcasted_iota(jnp.int32, (TILE, TILE), 1)
        down = lax.broadcasted_iota(jnp.int32, (TILE, TILE), 0)
        rows = jnp.broadcast_to(IX[0:1, :], (TILE, TILE))
        cols = jnp.broadcast_to(IX[8:9, :], (TILE, TILE))
        live = lane < count[0, 0]
        for which, key in enumerate((rows * KBLOCKS + cols, cols * IBLOCKS + rows)):
            shift = 5 if which == 0 else 4
            key = jnp.where(live, key, FAR + lane)
            key_down = key.T
            own, other = key_down >> shift, key_down & ((1 << shift) - 1)
            less = key < key_down
            rank = jnp.sum(jnp.where(less, 1, 0), axis=1, keepdims=True)
            same = less & ((key >> shift) == own)
            keep = jnp.minimum(jnp.sum(jnp.where(same, 1, 0), axis=1, keepdims=True), 1)
            if which == 0:
                piece = other >> 1
                dy = ((piece >> 2) + SIDE - y) & 3
                dz = (piece + SIDE - z) & 3
                place = (dy * SIDE + dz) * 2 + (other & 1)
            else:
                to_col = other >> 1
                dx = (turn * ((to_col >> 1) - x)) & 3
                dk = (to_col + 2 - k) & 1
                place = (dk * SIDE + dx) * 2 + (other & 1)
            hit = rank == lane
            upto = jnp.sum(jnp.where(own <= lane, 1, 0), axis=0, keepdims=True)
            any_own = jnp.sum(jnp.where(own == lane, 1, 0), axis=0, keepdims=True)
            at = which * 8
            TV[at : at + 1, :] = jnp.sum(jnp.where(hit, down, 0), axis=0, keepdims=True)
            TV[at + 1 : at + 2, :] = jnp.sum(jnp.where(hit, place, 0), axis=0, keepdims=True)
            TV[at + 2 : at + 3, :] = jnp.sum(jnp.where(hit, keep, 0), axis=0, keepdims=True)
            TV[at + 3 : at + 4, :] = jnp.where(any_own > 0, upto - 1, SLOTS)

    def tables_1():
        copy = pltpu.make_async_copy(TV, TS, lsem.at[LOCAL])
        copy.start()
        copy.wait()

    def product(c, which, part):
        at = which * 8
        base = part * SLOTS_AT_ONCE
        total = None if part == 0 else Z[c][base - 1]
        for slot in range(base, base + SLOTS_AT_ONCE):
            place = TS[at + 1, slot]
            block = (BK if which == 0 else BT)[TS[at, slot]]
            value = jnp.dot(block, (G if which == 0 else DG)[c][place], preferred_element_type=F32)
            if total is not None:
                value = value + total * TS[at + 2, slot].astype(F32)
            Z[c][slot] = value
            total = value

    def multiply(c, part):
        product(c, 0, part)

    def multiply_back(c, part):
        product(c, 1, part)

    def part_of(c, dk, dx):
        row = (((x + turn * dx + SIDE) % SIDE) * 2 + (k + dk) % 2) * 2
        return jnp.concatenate([Z[c][TS[3, row]], Z[c][TS[3, row + 1]]], axis=0)

    def reduce_0(c):
        for dx in (2, 3, 1, 0):
            S1[c][dx] = part_of(c, 1, dx).astype(BF16)
            mirrored = wrap(-dx)
            send(("c0", c, mirrored), S1[c].at[dx], R0[c].at[mirrored], dev(dk=1))

    def paired(c, dx):
        take(("c0", c, dx), 2)
        return part_of(c, 0, dx) + R0[c][dx].astype(F32)

    def reduce_1(c):
        XS[c][0] = paired(c, 2).astype(BF16)
        if c in DIRECT_SUMS:
            send(("cr", c), XS[c].at[0], XR[c].at[0], dev(dx=2))
        else:
            for half in range(2):
                lines = pl.ds(half * TILE, TILE)
                send(("cf", c, half), XS[c].at[0, lines], XR[c].at[0, lines], dev(dx=turn))
        XS[c][1] = paired(c, 3).astype(BF16)
        send(("cr", c), XS[c].at[1], XR[c].at[1], dev(dx=-turn))
        if c in DIRECT_SUMS:
            XS[c][2] = paired(c, 1).astype(BF16)
            send(("cr", c), XS[c].at[2], XR[c].at[2], dev(dx=turn))

    def reduce_2(c):
        if c in DIRECT_SUMS:
            return
        value = paired(c, 1)
        for half in range(2):
            lines = pl.ds(half * TILE, TILE)
            part = value[half * TILE : (half + 1) * TILE]
            take(("cf", c, half), 1)
            XS[c][2, lines] = (part + XR[c][0, lines].astype(F32)).astype(BF16)
            send(("cr", c), XS[c].at[2, lines], XR[c].at[2, lines], dev(dx=turn))

    def reduce_3(c):
        value = paired(c, 0)
        take(("cr", c), 6 if c in DIRECT_SUMS else 4)
        for n in range(0 if c in DIRECT_SUMS else 1, 3):
            value = value + XR[c][n].astype(F32)
        HD[:, STARTS[c] : STARTS[c] + WIDTHS[c]] = value.astype(BF16)

    def turn_blocks(part):
        @pl.loop(0, SLOTS_AT_ONCE // 4)
        def _(n):
            for j in range(4):
                s = part * SLOTS_AT_ONCE + n * 4 + j
                BT[s] = BK[s].T

    def run(order, table):
        for name, *args in order:
            table[name](*args)

    def prepare():
        tables_0()
        blocks_in.wait()
        turn_blocks(0)
        tables_1()

    def multiply_all(c):
        gather_8(c)
        for part in range(3):
            multiply(c, part)
        reduce_0(c)

    steps = dict(g0=gather_0, own=gather_own, g1=gather_1, g2=gather_2, g3=gather_3, g4=gather_4)
    steps.update(g6=gather_6, mm=multiply_all, r1=reduce_1, r2=reduce_2, r3=reduce_3)
    steps.update(prep=prepare, turn=turn_blocks)
    run(FORWARD, steps)
    weight_in.wait()
    ups_in.wait()

    bias_rows = []
    bias_in.wait()
    for n in range(2):
        columns = slice(n * HALF, (n + 1) * HALF)
        pre = jnp.dot(HD[...], WT[:, columns], preferred_element_type=F32) + BV[:, columns]
        sig = jax.nn.sigmoid(pre)
        AO[:, columns] = (pre * sig).astype(BF16)
        dpre = (UP[:, columns].astype(F32) * sig * (1.0 + pre * (1.0 - sig))).astype(BF16)
        DP[:, columns] = dpre
        bias_rows.append(jnp.sum(dpre.astype(F32).reshape(32, 8, HALF), axis=0))

    def hidden(c, place):
        return DG[c].at[pl.ds(2 * place, 2)]

    def spread_0(c):
        value = lax.dot_general(
            DP[...],
            WT[pl.ds(STARTS[c], WIDTHS[c]), :],
            (((1,), (1,)), ((), ())),
            preferred_element_type=F32,
        )
        DG[c][0:2] = value.astype(BF16).reshape(2, TILE, WIDTHS[c])
        if c in DIRECT_SPREAD:
            send(("sr", c), hidden(c, 0), hidden(c, 2), dev(dx=2))
            send(("sp", c), hidden(c, 0), hidden(c, 3), dev(dx=turn))
        else:
            for half in range(2):
                send(("sp", c, half), DG[c].at[half], DG[c].at[6 + half], dev(dx=turn))
        send(("sm", c), hidden(c, 0), hidden(c, 1), dev(dx=-turn))
        send(("sc", c), hidden(c, 0), hidden(c, SIDE), dev(dk=1))

    def spread_1(c):
        if c in DIRECT_SPREAD:
            take(("sp", c), 2)
        else:
            for half in range(2):
                take(("sp", c, half), 1)
                send(("sr", c), DG[c].at[6 + half], DG[c].at[4 + half], dev(dx=turn))
        send(("sc", c), hidden(c, 3), hidden(c, SIDE + 1), dev(dk=1))
        take(("sm", c), 2)
        send(("sc", c), hidden(c, 1), hidden(c, SIDE + 3), dev(dk=1))

    def spread_2(c):
        take(("sr", c), 2)
        send(("sc", c), hidden(c, 2), hidden(c, SIDE + 2), dev(dk=1))

    def spread_3(c):
        take(("sc", c), 8)

    plane = [(dy, dz) for dy in range(SIDE) for dz in range(SIDE) if dy or dz]

    def weight_0():
        value = lax.dot_general(
            HD[...], DP[...], (((0,), (0,)), ((), ())), preferred_element_type=F32
        )
        for zz in range(SIDE):
            lanes = slice(zz * TILE, (zz + 1) * TILE)
            tiles = value[:, lanes].reshape(2, SIDE, SIDE, 16, TILE)
            sums = bias_rows[zz // 2][:, (zz % 2) * TILE : (zz % 2 + 1) * TILE]
            for yy in range(SIDE):
                GP[:, yy * SIDE + zz, :, 0:16, :] = tiles[:, :, yy]
                GP[:, yy * SIDE + zz, :, 16:24, :] = jnp.broadcast_to(
                    sums, (2, SIDE, 8, TILE)
                )
        send(("wk",), GP.at[1 - k], AK, dev(dk=1), out=CHUNKS + 0)

    def weight_1():
        wait_bytes(AK, rsem.at[groups[("wk",)]])
        AK[...] = GP[k] + AK[...]
        PX[...] = AK[...].astype(BF16)
        for n, (dy, dz) in enumerate(plane):
            there = ((y + dy) % SIDE) * SIDE + (z + dz) % SIDE
            send(("wp",), PX.at[there], PR.at[n], dev(dy=dy, dz=dz), out=CHUNKS + 1)

    def weight_2():
        wait_bytes(PR, rsem.at[groups[("wp",)]])
        value = AK[ri]
        for n in range(len(plane)):
            value = value + PR[n].astype(F32)
        XA[...] = value
        for n in (2, 1, 3):
            send(("wx",), XA.at[(x + n) % SIDE], XB.at[n - 1], dev(dx=n), out=CHUNKS + 2)

    def weight_3():
        wait_bytes(XB, rsem.at[groups[("wx",)]])
        value = XA[x]
        for n in range(3):
            value = value + XB[n]
        FK[k, x, ri] = (value * scale).astype(BF16)
        mine = FK.at[k, x, ri]
        for dy, dz in plane:
            send(("vp",), mine, mine, dev(dy=dy, dz=dz), out=CHUNKS + 3)

    def weight_4():
        wait_bytes(LIKE, rsem.at[groups[("vp",)]])
        mine = FK.at[k, x]
        for n in (2, 1, 3):
            send(("vx",), mine, mine, dev(dx=n), out=CHUNKS + 4)

    def weight_5():
        wait_bytes(FK.at[0, pl.ds(0, 3)], rsem.at[groups[("vx",)]])
        send(("vk",), FK.at[k], FK.at[k], dev(dk=1), out=CHUNKS + 5)

    def weight_6():
        wait_bytes(FK.at[0], rsem.at[groups[("vk",)]])
        for yy in range(SIDE):
            for zz in range(SIDE):
                lanes = slice(zz * TILE, (zz + 1) * TILE)
                for kk in range(2):
                    for xx in range(SIDE):
                        first = kk * 256 + xx * 64 + yy * 16
                        WO[first : first + 16, lanes] = FK[kk, xx, yy * SIDE + zz, 0:16, :].astype(F32)
        for zz in range(SIDE):
            BO[:, zz * TILE : (zz + 1) * TILE] = jnp.sum(
                FK[0, 0, zz, 16:24, :].astype(F32), axis=0, keepdims=True
            )

    def offset(c, name):
        e = first_way(c)
        return {"far": 2, "relay": e, "near": -e, "mine": 0}[name]

    def group_way(name):
        return 1 if name in ("far", "mine") else -1

    def sum_of(c, h, a, b):
        dy, dz = (a, b) if h == 0 else (b, a)
        column = (((y + dy + SIDE) % SIDE) * SIDE + (z + dz + SIDE) % SIDE) * 2 + h
        return Z[c][TS[8 + 3, column]]

    NAMES = ("far", "relay", "near", "mine")

    def back_0(c, i):
        name = NAMES[i]
        a, e = offset(c, name), group_way(name)
        for h in range(2):
            SB[c][h, i, 0] = sum_of(c, h, a, 2).astype(BF16)
            send(("bf", c, i), SB[c].at[h, i, 0], SR[c].at[h, i, 0], along(h, False, e))
        for h in range(2):
            SB[c][h, i, 1] = sum_of(c, h, a, -e).astype(BF16)
            send(("br", c, i), SB[c].at[h, i, 1], SR[c].at[h, i, 1], along(h, False, -e))

    def back_1(c, i):
        name = NAMES[i]
        a, e = offset(c, name), group_way(name)
        take(("bf", c, i), 2)
        for h in range(2):
            SB[c][h, i, 2] = (sum_of(c, h, a, e) + SR[c][h, i, 0].astype(F32)).astype(BF16)
            send(("br", c, i), SB[c].at[h, i, 2], SR[c].at[h, i, 2], along(h, False, e))

    def back_2(c, i):
        name = NAMES[i]
        e = first_way(c)
        take(("br", c, i), 4)
        if name == "relay" and c not in DIRECT_LAST:
            take(("tf", c), 2)
        for h in range(2):
            value = sum_of(c, h, offset(c, name), 0) + SR[c][h, i, 1].astype(F32)
            value = value + SR[c][h, i, 2].astype(F32)
            if name == "far":
                step = 2 if c in DIRECT_LAST else e
                SB[c][h, 4, 0] = value.astype(BF16)
                send(("tf", c), SB[c].at[h, 4, 0], SR[c].at[h, 4, 0], along(h, True, step))
            elif name == "near":
                SB[c][h, 4, 1] = value.astype(BF16)
                send(("tr", c), SB[c].at[h, 4, 1], SR[c].at[h, 4, 1], along(h, True, -e))
            elif name == "relay":
                if c not in DIRECT_LAST:
                    value = value + SR[c][h, 4, 0].astype(F32)
                SB[c][h, 4, 2] = value.astype(BF16)
                send(("tr", c), SB[c].at[h, 4, 2], SR[c].at[h, 4, 2], along(h, True, e))
            else:
                UK[c][h] = value

    def back_3(c):
        take(("tr", c), 4)
        if c in DIRECT_LAST:
            take(("tf", c), 2)
        for h in range(2):
            value = UK[c][h] + SR[c][h, 4, 1].astype(F32)
            value = value + SR[c][h, 4, 2].astype(F32)
            if c in DIRECT_LAST:
                value = value + SR[c][h, 4, 0].astype(F32)
            FO[h * TILE : (h + 1) * TILE, STARTS[c] : STARTS[c] + WIDTHS[c]] = value.astype(BF16)

    def multiply_back_all(c):
        spread_3(c)
        for part in range(3):
            multiply_back(c, part)

    steps = dict(w0=weight_0, w1=weight_1, w2=weight_2, w3=weight_3, w4=weight_4, w5=weight_5)
    steps.update(w6=weight_6, s0=spread_0, s1=spread_1, s2=spread_2, mm=multiply_back_all)
    steps.update(b0=back_0, b1=back_1, b2=back_2, b3=back_3)
    run(BACKWARD, steps)

    assert len(groups) == GROUPS, len(groups)
    for c in range(CHUNKS):
        wait_bytes(Z[c].at[pl.ds(0, 44)], ssem.at[c])
    for number, like in enumerate(
        (AK, PR, XB, LIKE, FK.at[0, pl.ds(0, 3)], FK.at[0]), start=CHUNKS
    ):
        wait_bytes(like, ssem.at[number])


def finish_kernel(a, b, c, d, ao, bo, co, do, sem):
    pairs = ((c, co), (a, ao), (b, bo), (d, do))
    copies = [pltpu.make_async_copy(p[0], p[1], sem.at[n]) for n, p in enumerate(pairs)]
    for copy in copies:
        copy.start()
    for copy in copies:
        copy.wait()


def shards(features, blocks, block_rows, block_cols, block_count, weight, bias_vector, upstream):
    scale = 1.0 / math.sqrt(features.shape[0] * SIDE * SIDE * SIDE * 2)
    vmem = pl.BlockSpec(memory_space=pltpu.VMEM)
    hbm = pl.BlockSpec(memory_space=pltpu.HBM)
    smem = pl.BlockSpec(memory_space=pltpu.SMEM)
    shapes = (
        jax.ShapeDtypeStruct((256, 512), BF16),
        jax.ShapeDtypeStruct((256, 512), BF16),
        jax.ShapeDtypeStruct((512, 512), F32),
        jax.ShapeDtypeStruct((1, 512), F32),
    )
    results = pl.pallas_call(
        functools.partial(step_kernel, scale),
        out_shape=shapes,
        in_specs=[smem] + [hbm] * 7,
        out_specs=(vmem, vmem, vmem, vmem),
        scratch_shapes=[
            *[pltpu.VMEM((KBLOCKS, TILE, w), BF16) for w in WIDTHS],
            *[pltpu.VMEM((SLOTS + 1, TILE, w), F32) for w in WIDTHS],
            *[pltpu.VMEM((IBLOCKS, TILE, w), BF16) for w in WIDTHS],
            *[pltpu.VMEM((SIDE, 256, w), BF16) for w in WIDTHS],
            *[pltpu.VMEM((SIDE, 256, w), BF16) for w in WIDTHS],
            *[pltpu.VMEM((3, 256, w), BF16) for w in WIDTHS],
            *[pltpu.VMEM((3, 256, w), BF16) for w in WIDTHS],
            *[pltpu.VMEM((2, TILE, w), F32) for w in WIDTHS],
            *[pltpu.VMEM((2, 5, 3, TILE, w), BF16) for w in WIDTHS],
            *[pltpu.VMEM((2, 5, 3, TILE, w), BF16) for w in WIDTHS],
            pltpu.VMEM((SLOTS, TILE, TILE), BF16),
            pltpu.VMEM((SLOTS, TILE, TILE), BF16),
            pltpu.VMEM((512, 512), BF16),
            pltpu.VMEM((256, 512), BF16),
            pltpu.VMEM((256, 512), BF16),
            pltpu.VMEM((256, 512), BF16),
            pltpu.VMEM((2, 16, SIDE, 24, TILE), F32),
            pltpu.VMEM((16, SIDE, 24, TILE), F32),
            pltpu.VMEM((16, SIDE, 24, TILE), BF16),
            pltpu.VMEM((15, SIDE, 24, TILE), BF16),
            pltpu.VMEM((SIDE, 24, TILE), F32),
            pltpu.VMEM((3, 24, TILE), F32),
            pltpu.VMEM((2, SIDE, 16, 24, TILE), BF16),
            pltpu.VMEM((15, 24, TILE), BF16),
            pltpu.VMEM((1, SLOTS), jnp.int32),
            pltpu.VMEM((1, SLOTS), jnp.int32),
            pltpu.VMEM((1, 512), F32),
            pltpu.VMEM((16, TILE), jnp.int32),
            pltpu.VMEM((16, TILE), jnp.int32),
            pltpu.SMEM((16, TILE), jnp.int32),
            pltpu.SemaphoreType.DMA((LOCAL + 1,)),
            pltpu.SemaphoreType.DMA((CHUNKS + 6,)),
            pltpu.SemaphoreType.DMA((GROUPS,)),
        ],
        compiler_params=pltpu.CompilerParams(
            collective_id=0, has_side_effects=True, vmem_limit_bytes=46 * 2**20
        ),
        name="graph_layer",
    )(
        block_count,
        *[
            pltpu.with_memory_space_constraint(array, pltpu.HBM)
            for array in (
                block_rows[0],
                block_cols[0],
                features,
                blocks[0, 0],
                weight,
                bias_vector.reshape(1, 512),
                upstream,
            )
        ],
    )
    activated, grad_features, grad_weight, grad_bias = pl.pallas_call(
        finish_kernel,
        out_shape=shapes,
        in_specs=[vmem] * 4,
        out_specs=(hbm,) * 4,
        scratch_shapes=[pltpu.SemaphoreType.DMA((4,))],
        compiler_params=pltpu.CompilerParams(vmem_limit_bytes=2 * 2**20),
        name="finish",
    )(*results)
    return (activated, grad_weight, grad_bias.reshape(512), grad_features)


def solution(mesh):
    in_specs = (
        P(("col", "row"), None),
        P("row", "col", None, None, None),
        P("row", "col", None),
        P("row", "col", None),
        P("row", "col"),
        P(),
        P(),
        P(("row", "col"), None),
    )
    out_specs = (P(("row", "col"), None), P(), P(), P(("col", "row"), None))
    return jax.shard_map(shards, mesh=mesh, in_specs=in_specs, out_specs=out_specs, check_vma=False)
```
